256 devices in a mesh: row: 16 (over y, x), col: 16 (over z, core).
Axes of the slice: x: 4, y: 4, z: 8, core: 2. Of those that a mesh axis runs over, the one named last changes fastest.
Arguments:
- coeffs: bfloat16 [16384, 2048], P('row'), may hold values from -1 to 1
- p_slots: int32 [16, 16, 8], P('row', 'col'), may hold values from 0 to 63, as said below
- p_count: int32 [16, 16], P('row', 'col'), may hold values from 1 to 8
- s_blocks: bfloat16 [16, 16, 8, 128, 128], P('row', 'col'), may hold values from -0.3984375 to 0.3984375
- s_slots: int32 [16, 16, 8], P('row', 'col'), may hold values from 0 to 63, as said below
- s_count: int32 [16, 16], P('row', 'col'), may hold values from 1 to 8
- q_slots: int32 [16, 16, 8], P('row', 'col'), may hold values from 0 to 63, as said below
- q_count: int32 [16, 16], P('row', 'col'), may hold values from 1 to 8
Outputs:
- density: bfloat16 [16, 16, 8, 128, 128], P('row', 'col')
- product: float32 [16, 16, 8, 128, 128], P('row', 'col')
The draws below stay inside these ranges and needn't reach their ends.
Inputs may be any that keep to these rules, and one draw needn't show every extreme that they name: `p_slots`: on each device the live slots name different blocks of its tile; at least one device has all 8 slots live, which one is drawn. `s_slots`: on each device the live slots name different positions; at least one device has all 8 slots live, which one is drawn. `q_slots`: on each device the live slots name different blocks of its tile; at least one device has all 8 slots live, which one is drawn.
All inputs are finite; a program needn't handle non-finite values.
Results may differ from the reference program's by a relative error of at most 0.0029.
Values may be sent and summed in bfloat16 or wider, within the bound.
A program may use at most 192 MiB of HBM per device.

```python
import jax
import jax.numpy as jnp
from jax import lax

N = 16384
K = 2048
ROWB = 8
COLB = 8
SPAN = 1
PMAX = 8
QMAX = 8
SMAX = 8
N_ROW = 16
N_COL = 16


def pattern_slots(key, total, most):
    keys = jax.random.split(key, N_ROW * N_COL)
    picks = jax.vmap(lambda single: jax.random.permutation(single, total)[:most])(keys)
    return picks.reshape(N_ROW, N_COL, most).astype(jnp.int32)


def pattern_count(key, most):
    first_key, second_key = jax.random.split(key)
    counts = jax.random.randint(first_key, (N_ROW * N_COL,), 1, most + 1)
    chosen = jax.random.randint(second_key, (), 0, N_ROW * N_COL)
    counts = jnp.where(jnp.arange(N_ROW * N_COL) == chosen, most, counts)
    return counts.reshape(N_ROW, N_COL).astype(jnp.int32)


def draw_p_slots(key, part):
    return pattern_slots(jax.random.fold_in(key, 11), ROWB * COLB, PMAX)


def draw_p_count(key, part):
    return pattern_count(jax.random.fold_in(key, 12), PMAX)


def draw_s_slots(key, part):
    return pattern_slots(jax.random.fold_in(key, 21), SPAN * COLB * COLB, SMAX)


def draw_s_count(key, part):
    return pattern_count(jax.random.fold_in(key, 22), SMAX)


def draw_q_slots(key, part):
    return pattern_slots(jax.random.fold_in(key, 31), ROWB * COLB, QMAX)


def draw_q_count(key, part):
    return pattern_count(jax.random.fold_in(key, 32), QMAX)


def level_of(stream_key, shape, cuts, low, largest):
    def one(dim, blocks):
        steps = jax.random.uniform(jax.random.fold_in(jax.random.fold_in(stream_key, 6), dim), (blocks,), jnp.float32, low / len(cuts), largest / len(cuts))
        return jnp.repeat(jnp.exp(steps), shape[dim] // blocks).reshape((-1,) + (1,) * (len(shape) - dim - 1))

    gain = one(*cuts[0])
    for cut in cuts[1:]:
        gain = gain * one(*cut)
    return gain


def gaussian(own_key, extent, deviation, limit, shards=(), kind=jnp.bfloat16):
    array = jax.random.normal(own_key, extent, jnp.float32) * deviation
    if len(shards) > 0:
        array = level_of(own_key, extent, shards, -0.22, 0.18) * array
    return jnp.clip(array, min=-limit, max=limit).astype(kind)


def setup_inputs(seed: int = 0) -> dict:
    key_list = jax.random.split(jax.random.key(seed), 9)
    return {
        "coeffs": gaussian(key_list[0], (N, K), 0.15, 1.0, ((0, 16),)),
        "p_slots": draw_p_slots(jax.random.fold_in(key_list[8], 71), 0),
        "p_count": draw_p_count(jax.random.fold_in(key_list[8], 71), 0),
        "s_blocks": gaussian(key_list[3], (N_ROW, N_COL, SMAX, 128, 128), 0.0625, 0.3984375, ((0, 16), (1, 16))),
        "s_slots": draw_s_slots(jax.random.fold_in(key_list[8], 71), 0),
        "s_count": draw_s_count(jax.random.fold_in(key_list[8], 71), 0),
        "q_slots": draw_q_slots(jax.random.fold_in(key_list[8], 71), 0),
        "q_count": draw_q_count(jax.random.fold_in(key_list[8], 71), 0),
    }


def reference(coeffs, p_slots, p_count, s_blocks, s_slots, s_count, q_slots, q_count):
    block_count = coeffs.shape[0] // 128
    orbitals = coeffs.shape[1]
    tile_rows = block_count // N_ROW
    tile_cols = block_count // N_COL
    grid_row = jnp.arange(N_ROW, dtype=jnp.int32)[:, None, None]
    grid_col = jnp.arange(N_COL, dtype=jnp.int32)[None, :, None]
    blocked = coeffs.reshape(block_count, 128, orbitals)

    p_live = jnp.arange(p_slots.shape[2], dtype=jnp.int32)[None, None, :] < p_count[:, :, None]
    p_global_row = (grid_row * tile_rows + p_slots // tile_cols).astype(jnp.int32).reshape(-1)
    p_global_col = (grid_col * tile_cols + p_slots % tile_cols).astype(jnp.int32).reshape(-1)

    def density_block(pair):
        return jnp.dot(blocked[pair[0]], blocked[pair[1]].T, preferred_element_type=jnp.float32)

    raw = lax.map(density_block, (p_global_row, p_global_col))
    raw = raw.reshape(N_ROW, N_COL, -1, 128, 128)
    density = jnp.where(p_live[..., None, None], raw, jnp.zeros_like(raw)).astype(jnp.bfloat16)

    dense_p = jnp.zeros((block_count, block_count, 128, 128), jnp.bfloat16)
    dense_p = dense_p.at[p_global_row, p_global_col].add(density.reshape(-1, 128, 128))

    s_live = jnp.arange(s_slots.shape[2], dtype=jnp.int32)[None, None, :] < s_count[:, :, None]
    local_row = s_slots // tile_cols
    panel_index = grid_row + N_ROW * (local_row // tile_cols)
    s_global_row = (panel_index * tile_cols + local_row % tile_cols).astype(jnp.int32).reshape(-1)
    s_global_col = (grid_col * tile_cols + s_slots % tile_cols).astype(jnp.int32).reshape(-1)
    s_kept = jnp.where(s_live[..., None, None], s_blocks, jnp.zeros_like(s_blocks)).reshape(-1, 128, 128)
    dense_s = jnp.zeros((block_count, block_count, 128, 128), jnp.bfloat16)
    dense_s = dense_s.at[s_global_row, s_global_col].add(s_kept)

    q_live = jnp.arange(q_slots.shape[2], dtype=jnp.int32)[None, None, :] < q_count[:, :, None]
    q_global_row = (grid_row * tile_rows + q_slots // tile_cols).astype(jnp.int32).reshape(-1)
    q_global_col = (grid_col * tile_cols + q_slots % tile_cols).astype(jnp.int32).reshape(-1)

    def product_block(pair):
        left = dense_p[pair[0]].astype(jnp.float32)
        right = dense_s[:, pair[1]].astype(jnp.float32)
        return jnp.einsum('kab,kbc->ac', left, right)

    summed = lax.map(product_block, (q_global_row, q_global_col))
    summed = summed.reshape(N_ROW, N_COL, -1, 128, 128)
    product = jnp.where(q_live[..., None, None], summed, jnp.zeros_like(summed))
    return density, product
```

```python
import functools

import jax
import jax.numpy as jnp
from jax import lax
from jax.experimental import pallas as pl
from jax.experimental.pallas import tpu as pltpu
from jax.sharding import PartitionSpec as P

MESH = pl.DeviceIdType.MESH
B = 128
OFFSETS = (0, 14, 8, 10, 12, 5, 2, 7, 13, 4, 9, 15, 6, 3, 11, 1)
INVERSE = tuple(OFFSETS.index(o) for o in range(16))


def lookup(table, at):
    value = 0
    for base in range(0, 16, 4):
        packed = sum(table[base + i] << (4 * i) for i in range(4))
        inside = (at // 4 == base // 4).astype(jnp.int32)
        value = value + inside * ((packed // (1 << (4 * (at % 4)))) % 16)
    return value


class Link:
    def __init__(self, send, recv, at):
        self.send, self.recv, self.at = send, recv, at
        self.sent = None

    def start(self, src, dst, device):
        self.sent = pltpu.make_async_remote_copy(
            src_ref=src, dst_ref=dst, send_sem=self.send.at[self.at], recv_sem=self.recv.at[self.at],
            device_id=device, device_id_type=MESH,
        )
        self.sent.start()

    def arrived(self, landing, device):
        pltpu.make_async_remote_copy(
            src_ref=landing, dst_ref=landing, send_sem=self.send.at[self.at], recv_sem=self.recv.at[self.at],
            device_id=device, device_id_type=MESH,
        ).wait_recv()


class PlaneGather:
    def __init__(self, buf, own, send, recv, place):
        self.buf, self.own = buf, own
        self.y, self.x, self.col = place
        self.rows = own.shape[0]
        self.links = [Link(send, recv, m) for m in range(40)]

    def coords(self, half, du, dv):
        if half == 0:
            return (self.y + dv + 4) % 4, (self.x + du + 4) % 4
        return (self.y + du + 4) % 4, (self.x + dv + 4) % 4

    def index(self, half, du, dv):
        y, x = self.coords(half, du, dv)
        return 4 * y + x

    def device(self, half, du, dv):
        return (self.index(half, du, dv), self.col)

    def span(self, half, part):
        size = self.rows // 2
        base = half * size
        if part is None:
            return pl.ds(base, size)
        return pl.ds(base + part * (size // 2), size // 2)

    def block(self, half, du, dv, part=None):
        return self.buf.at[self.index(half, du, dv), self.span(half, part)]

    def link(self, half, number):
        return self.links[20 * half + number]

    def first(self, half):
        src = self.own.at[self.span(half, None)]
        dst = self.block(half, 0, 0)
        self.link(half, 0).start(src, dst, self.device(half, 1, 0))
        self.link(half, 1).start(src, dst, self.device(half, -1, 0))

    def relay_first(self, half, side):
        du = -1 if side == 0 else 1
        self.link(half, side).arrived(self.block(half, du, 0), self.device(half, du, 0))
        part = self.block(half, du, 0, side)
        self.link(half, 2 + side).start(part, part, self.device(half, -du, 0))

    def far_first(self, half):
        for side in range(2):
            part = self.block(half, 2, 0, side)
            self.link(half, 2 + side).arrived(part, self.device(half, -1 if side == 0 else 1, 0))

    def second(self, half, j):
        du = (0, -1, 1, 2)[j]
        dst = self.block(half, du, 0)
        src = self.own.at[self.span(half, None)] if j == 0 else dst
        self.link(half, 4 + 4 * j).start(src, dst, self.device(half, 0, 1))
        self.link(half, 5 + 4 * j).start(src, dst, self.device(half, 0, -1))

    def relay_second(self, half, j, side):
        du = (0, -1, 1, 2)[j]
        dv = -1 if side == 0 else 1
        number = 4 + 4 * j + side
        self.link(half, number).arrived(self.block(half, du, dv), self.device(half, 0, dv))
        part = self.block(half, du, dv, side)
        self.link(half, number + 2).start(part, part, self.device(half, 0, -dv))

    def far_second(self, half, j):
        du = (0, -1, 1, 2)[j]
        for side in range(2):
            part = self.block(half, du, 2, side)
            self.link(half, 6 + 4 * j + side).arrived(part, self.device(half, 0, -1 if side == 0 else 1))

    def finish(self):
        for link in self.links:
            link.sent.wait_send()


def gather_kernel(
    coeffs, sblk, p_slots, p_count, s_slots, s_count, q_slots, q_count,
    dens, pall, sall, sidx,
    own, pan, sown, pcode, scode,
    local_sem, scat_sem, c_send, c_recv, g_send, g_recv, s_send, s_recv, z_send, z_recv,
):
    row = lax.axis_index("row")
    col = lax.axis_index("col")
    y, x = row // 4, row % 4
    z, k = col // 2, col % 2

    load_own = pltpu.make_async_copy(coeffs, own, local_sem.at[0])
    load_s = pltpu.make_async_copy(sblk, sown, local_sem.at[1])
    load_own.start()
    load_s.start()

    serve = 2 * ((z - row // 2 + 8) % 8) + (k + row) % 2
    offset = lookup(OFFSETS, serve)
    dest_row = 4 * ((y + offset // 4) % 4) + (x + offset % 4) % 4
    back = 4 * ((y - col // 4 + 4) % 4) + (x - col % 4 + 4) % 4
    served = lookup(INVERSE, back)
    source_col = 2 * ((col // 2 + served // 2) % 8) + (served + col) % 2
    mine = row == col

    barrier = pltpu.get_barrier_semaphore()
    for j in range(1, 16):
        pl.semaphore_signal(barrier, inc=1, device_id=(row, (col + j) % 16), device_id_type=MESH)
        pl.semaphore_signal(barrier, inc=1, device_id=((row + j) % 16, col), device_id_type=MESH)

    @pl.when(serve != 0)
    def _():
        pl.semaphore_signal(barrier, inc=1, device_id=(dest_row, row), device_id_type=MESH)

    @pl.when(back != 0)
    def _():
        pl.semaphore_signal(barrier, inc=1, device_id=(col, source_col), device_id_type=MESH)

    lane = lax.broadcasted_iota(jnp.int32, (8, B), 1)
    sub = lax.broadcasted_iota(jnp.int32, (8, B), 0)
    pc = jnp.full((8, B), -1, jnp.int32)
    qc = jnp.full((8, B), -100, jnp.int32)
    sc = jnp.full((8, B), -1, jnp.int32)
    p_live = jnp.full((8, B), p_count[0], jnp.int32)
    q_live = jnp.full((8, B), q_count[0], jnp.int32)
    s_live = jnp.full((8, B), s_count[0], jnp.int32)
    for i in range(8):
        pc = jnp.where((lane // 8 == i) & (p_live > i), jnp.full((8, B), p_slots[i], jnp.int32), pc)
        qc = jnp.where(
            (lane % 8 == i) & (lane < 64) & (q_live > i), jnp.full((8, B), q_slots[i], jnp.int32), qc
        )
        sc = jnp.where((sub == i) & (s_live > i), jnp.full((8, B), s_slots[i], jnp.int32), sc)
    pcode[col] = pc
    scode[row] = sc

    load_own.wait()
    load_s.wait()

    @pl.when(serve != 0)
    def _():
        pl.semaphore_wait(barrier, 32)

    @pl.when(serve == 0)
    def _():
        pl.semaphore_wait(barrier, 30)

    def scatter_copy(target_row, device):
        return pltpu.make_async_remote_copy(
            src_ref=own.at[:, :, pl.ds(pl.multiple_of(target_row * B, B), B)],
            dst_ref=pan.at[target_row],
            send_sem=scat_sem.at[0], recv_sem=scat_sem.at[1], device_id=device, device_id_type=MESH,
        )

    @pl.when(serve != 0)
    def _():
        scatter_copy(dest_row, (dest_row, row)).start()

    @pl.when(serve == 0)
    def _():
        pltpu.make_async_copy(
            own.at[:, :, pl.ds(pl.multiple_of(row * B, B), B)], pan.at[row], scat_sem.at[0]
        ).start()

    place = (y, x, col)
    panel = PlaneGather(pan, pan.at[row], c_send, c_recv, place)
    inter = PlaneGather(sall, sown, s_send, s_recv, place)

    for half in range(2):
        inter.first(half)
    keep_s = pltpu.make_async_copy(sown, sall.at[row], local_sem.at[2])
    keep_s.start()

    codes = []
    for j in range(1, 16):
        link = Link(g_send, g_recv, 2 * j - 2)
        link.start(pcode.at[col], pcode.at[col], (row, (col + j) % 16))
        codes.append(link)
        link = Link(g_send, g_recv, 2 * j - 1)
        link.start(scode.at[row], scode.at[row], ((row + j) % 16, col))
        codes.append(link)

    @pl.when(serve != 0)
    def _():
        scatter_copy(row, (col, source_col)).wait_recv()

    @pl.when(serve == 0)
    def _():
        pltpu.make_async_copy(
            own.at[:, :, pl.ds(pl.multiple_of(row * B, B), B)], pan.at[row], scat_sem.at[0]
        ).wait()

    for half in range(2):
        panel.first(half)
    for half in range(2):
        panel.second(half, 0)
    for side in range(2):
        for half in range(2):
            inter.relay_first(half, side)
    for side in range(2):
        for half in range(2):
            panel.relay_first(half, side)
            panel.second(half, 1 + side)
    for half in range(2):
        panel.far_first(half)
        panel.second(half, 3)

    for j in range(1, 16):
        codes[2 * j - 2].arrived(pcode.at[(col - j + 16) % 16], (row, (col - j + 16) % 16))
        codes[2 * j - 1].arrived(scode.at[(row - j + 16) % 16], ((row - j + 16) % 16, col))
    pcs, scs = pcode[...], scode[...]
    q = qc[None]
    match = ((pcs >> 3) == (q >> 3)) & ((scs >> 3) == (pcs & 7)) & ((scs & 7) == (q & 7))
    match = match & (pcs >= 0) & (scs >= 0) & (q >= 0)
    found = jnp.where(match, lax.broadcasted_iota(jnp.int32, (16, 8, B), 1) + 1, 0)
    found = jnp.sum(found, axis=1)
    total = jnp.sum((found > 0).astype(jnp.int32), axis=1, keepdims=True)
    sidx[...] = jnp.where(lax.broadcasted_iota(jnp.int32, (16, B), 1) == 64, total, found)

    for half in range(2):
        inter.far_first(half)
    for j in range(4):
        for side in range(2):
            for half in range(2):
                panel.relay_second(half, j, side)
    for j in range(4):
        for half in range(2):
            panel.far_second(half, j)

    for j in range(4):
        for half in range(2):
            inter.second(half, j)

    for s in range(8):
        a = p_slots[s] >> 3
        b = p_slots[s] & 7
        left = own[a]
        right = jnp.concatenate([pan[i, b] for i in range(16)], axis=1)
        raw = lax.dot_general(left, right, (((1,), (1,)), ((), ())), preferred_element_type=jnp.float32)
        raw = jnp.where(jnp.full((B, B), p_count[0], jnp.int32) > s, raw, 0.0)
        dens[s] = raw.astype(jnp.bfloat16)

    sibling = (row, col + 1 - 2 * k)
    up = (row, (col + 2) % 16)
    down = (row, (col + 14) % 16)
    half_rows = dens.shape[0] // 2
    ring = [Link(z_send, z_recv, m) for m in range(30)]

    def tile(at, chunk):
        return pall.at[at, pl.ds(chunk * half_rows, half_rows)]

    def number(way, distance, chunk):
        return 7 * way + (2 * (distance - 1) + chunk if distance < 4 else 6)

    for chunk in range(2):
        src = dens.at[pl.ds(chunk * half_rows, half_rows)]
        ring[number(0, 1, chunk)].start(src, tile(col, chunk), up)
        ring[number(1, 1, chunk)].start(src, tile(col, chunk), down)
    for chunk in range(2):
        ring[14 + chunk].start(dens.at[pl.ds(chunk * half_rows, half_rows)], tile(col, chunk), sibling)
    keep_p = pltpu.make_async_copy(dens, pall.at[col], local_sem.at[3])
    keep_p.start()

    def pass_on(way, distance, chunk):
        at = (col + 16 - 2 * distance) % 16 if way == 0 else (col + 2 * distance) % 16
        here = tile(at, chunk)
        me = number(way, distance, chunk)
        ring[me].arrived(here, down if way == 0 else up)
        if distance < 3 or (distance == 3 and chunk == way):
            ring[number(way, distance + 1, chunk)].start(here, here, up if way == 0 else down)
        ring[16 + me].start(here, here, sibling)

    def across(me, at, chunk):
        ring[me].arrived(tile(at, chunk), sibling)

    arrivals = [(d, c) for d in (1, 2, 3) for c in range(2)]
    relays = [(j, side) for j in range(4) for side in range(2)]
    for n in range(8):
        if n < 6:
            for way in range(2):
                pass_on(way, *arrivals[n])
        j, side = relays[n]
        for half in range(2):
            inter.relay_second(half, j, side)
    for way in range(2):
        pass_on(way, 4, way)
    for j in range(4):
        for half in range(2):
            inter.far_second(half, j)
    other = col + 1 - 2 * k
    for chunk in range(2):
        across(14 + chunk, other, chunk)
    for way in range(2):
        for distance in (1, 2, 3):
            for chunk in range(2):
                at = (other + 16 - 2 * distance) % 16 if way == 0 else (other + 2 * distance) % 16
                across(16 + number(way, distance, chunk), at, chunk)
        across(16 + number(way, 4, way), (other + 8) % 16, way)

    keep_s.wait()
    keep_p.wait()
    panel.finish()
    inter.finish()
    for link in codes + ring:
        link.sent.wait_send()

    @pl.when(serve != 0)
    def _():
        scatter_copy(dest_row, (dest_row, row)).wait_send()


def product_kernel(sidx, pall, sall, out, todo, pbuf, sbuf, count, sem_p, sem_s):
    depth = pbuf.shape[0]
    out[...] = jnp.zeros_like(out)
    count[0] = 0

    def scan(t, _):
        @pl.when(sidx[t, 64] > 0)
        def _():
            def inner(i, _):
                v = sidx[t, i]

                @pl.when(v > 0)
                def _():
                    n = count[0]
                    todo[n] = t * 1024 + i * 16 + v - 1
                    count[0] = n + 1

                return 0

            lax.fori_loop(0, 64, inner, 0)

        return 0

    lax.fori_loop(0, 16, scan, 0)
    n = count[0]

    def copies(i):
        code = todo[i]
        t, p, s = code // 1024, code // 128 % 8, code % 16
        at = i % depth
        return (
            pltpu.make_async_copy(pall.at[t, p], pbuf.at[at], sem_p.at[at]),
            pltpu.make_async_copy(sall.at[t, s], sbuf.at[at], sem_s.at[at]),
        )

    def begin(i, _):
        for copy in copies(i):
            copy.start()
        return 0

    lax.fori_loop(0, jnp.minimum(n, depth), begin, 0)

    def work(i, _):
        for copy in copies(i):
            copy.wait()
        at = i % depth
        q = todo[i] // 16 % 8
        out[q] += jnp.dot(pbuf[at], sbuf[at], preferred_element_type=jnp.float32)

        @pl.when(i + depth < n)
        def _():
            begin(i + depth, 0)

        return 0

    lax.fori_loop(0, n, work, 0)


def on_device(coeffs, p_slots, p_count, s_blocks, s_slots, s_count, q_slots, q_count):
    rows, orbitals = coeffs.shape
    n = 16
    smem = pl.BlockSpec(memory_space=pltpu.SMEM)
    vmem = pl.BlockSpec(memory_space=pltpu.VMEM)
    anyspace = pl.BlockSpec(memory_space=pl.ANY)
    gathered = jax.ShapeDtypeStruct((n, rows // B, B, B), jnp.bfloat16)
    dma = pltpu.SemaphoreType.DMA
    dens, pall, sall, sidx = pl.pallas_call(
        gather_kernel,
        out_shape=(
            jax.ShapeDtypeStruct((rows // B, B, B), jnp.bfloat16), gathered, gathered,
            jax.ShapeDtypeStruct((n, B), jnp.int32),
        ),
        in_specs=[anyspace, anyspace] + [smem] * 6,
        out_specs=(vmem, anyspace, anyspace, vmem),
        scratch_shapes=[
            pltpu.VMEM((rows // B, B, orbitals), jnp.bfloat16),
            pltpu.VMEM((n, rows // B, B, B), jnp.bfloat16),
            pltpu.VMEM((rows // B, B, B), jnp.bfloat16),
            pltpu.VMEM((n, 8, B), jnp.int32),
            pltpu.VMEM((n, 8, B), jnp.int32),
            dma((4,)), dma((2,)),
            dma((40,)), dma((40,)), dma((30,)), dma((30,)), dma((40,)), dma((40,)), dma((30,)), dma((30,)),
        ],
        compiler_params=pltpu.CompilerParams(collective_id=0, has_side_effects=True),
        name="gather",
    )(
        coeffs.reshape(rows // B, B, orbitals), s_blocks.reshape(rows // B, B, B), p_slots.reshape(8), p_count.reshape(1), s_slots.reshape(8),
        s_count.reshape(1), q_slots.reshape(8), q_count.reshape(1),
    )
    depth = 32
    product = pl.pallas_call(
        product_kernel,
        out_shape=jax.ShapeDtypeStruct((8, B, B), jnp.float32),
        in_specs=[smem, anyspace, anyspace],
        out_specs=vmem,
        scratch_shapes=[
            pltpu.SMEM((1024,), jnp.int32),
            pltpu.VMEM((depth, B, B), jnp.bfloat16),
            pltpu.VMEM((depth, B, B), jnp.bfloat16),
            pltpu.SMEM((1,), jnp.int32),
            dma((depth,)), dma((depth,)),
        ],
        name="product",
    )(sidx, pall, sall)
    return dens.reshape(1, 1, 8, B, B), product.reshape(1, 1, 8, B, B)


def solution(mesh):
    return jax.shard_map(
        on_device,
        mesh=mesh,
        in_specs=(
            P("row", None),
            P("row", "col", None),
            P("row", "col"),
            P("row", "col", None, None, None),
            P("row", "col", None),
            P("row", "col"),
            P("row", "col", None),
            P("row", "col"),
        ),
        out_specs=(P("row", "col", None, None, None), P("row", "col", None, None, None)),
        check_vma=False,
    )
```

```python
import functools

import jax
import jax.numpy as jnp
from jax import lax
from jax.experimental import pallas as pl
from jax.experimental.pallas import tpu as pltpu
from jax.sharding import PartitionSpec as P

MESH = pl.DeviceIdType.MESH
B = 128
FIRST = (8, 11, 6, 9, 14, 7, 10, 5)
SECOND = (2, 1, 12, 3, 4, 13, 0, 15)
PLANE = tuple((FIRST if i in FIRST else SECOND).index(i) for i in range(16))


def lookup(table, at):
    value = 0
    for base in range(0, len(table), 4):
        packed = sum(table[base + i] << (4 * i) for i in range(4))
        inside = (at // 4 == base // 4).astype(jnp.int32)
        value = value + inside * ((packed // (1 << (4 * (at % 4)))) % 16)
    return value


class Link:
    def __init__(self, send, recv, at):
        self.send, self.recv, self.at = send, recv, at
        self.sent = None

    def start(self, src, dst, device):
        self.sent = pltpu.make_async_remote_copy(
            src_ref=src, dst_ref=dst, send_sem=self.send.at[self.at], recv_sem=self.recv.at[self.at],
            device_id=device, device_id_type=MESH,
        )
        self.sent.start()

    def arrived(self, landing, device):
        pltpu.make_async_remote_copy(
            src_ref=landing, dst_ref=landing, send_sem=self.send.at[self.at], recv_sem=self.recv.at[self.at],
            device_id=device, device_id_type=MESH,
        ).wait_recv()


class PlaneGather:
    def __init__(self, buf, own, send, recv, place):
        self.buf, self.own = buf, own
        self.y, self.x, self.col = place
        self.rows = own.shape[0]
        self.links = [Link(send, recv, m) for m in range(40)]

    def coords(self, half, du, dv):
        if half == 0:
            return (self.y + dv + 4) % 4, (self.x + du + 4) % 4
        return (self.y + du + 4) % 4, (self.x + dv + 4) % 4

    def index(self, half, du, dv):
        y, x = self.coords(half, du, dv)
        return 4 * y + x

    def device(self, half, du, dv):
        return (self.index(half, du, dv), self.col)

    def span(self, half, part):
        size = self.rows // 2
        base = half * size
        if part is None:
            return pl.ds(base, size)
        return pl.ds(base + part * (size // 2), size // 2)

    def block(self, half, du, dv, part=None):
        return self.buf.at[self.index(half, du, dv), self.span(half, part)]

    def link(self, half, number):
        return self.links[20 * half + number]

    def first(self, half):
        src = self.own.at[self.span(half, None)]
        dst = self.block(half, 0, 0)
        self.link(half, 0).start(src, dst, self.device(half, 1, 0))
        self.link(half, 1).start(src, dst, self.device(half, -1, 0))

    def relay_first(self, half, side):
        du = -1 if side == 0 else 1
        self.link(half, side).arrived(self.block(half, du, 0), self.device(half, du, 0))
        part = self.block(half, du, 0, side)
        self.link(half, 2 + side).start(part, part, self.device(half, -du, 0))

    def far_first(self, half):
        for side in range(2):
            part = self.block(half, 2, 0, side)
            self.link(half, 2 + side).arrived(part, self.device(half, -1 if side == 0 else 1, 0))

    def second(self, half, j):
        du = (0, -1, 1, 2)[j]
        dst = self.block(half, du, 0)
        src = self.own.at[self.span(half, None)] if j == 0 else dst
        self.link(half, 4 + 4 * j).start(src, dst, self.device(half, 0, 1))
        self.link(half, 5 + 4 * j).start(src, dst, self.device(half, 0, -1))

    def relay_second(self, half, j, side):
        du = (0, -1, 1, 2)[j]
        dv = -1 if side == 0 else 1
        number = 4 + 4 * j + side
        self.link(half, number).arrived(self.block(half, du, dv), self.device(half, 0, dv))
        part = self.block(half, du, dv, side)
        self.link(half, number + 2).start(part, part, self.device(half, 0, -dv))

    def far_second(self, half, j):
        du = (0, -1, 1, 2)[j]
        for side in range(2):
            part = self.block(half, du, 2, side)
            self.link(half, 6 + 4 * j + side).arrived(part, self.device(half, 0, -1 if side == 0 else 1))

    def finish(self):
        for link in self.links:
            link.sent.wait_send()


def gather_kernel(
    coeffs, sblk, p_slots, p_count, s_slots, s_count, q_slots, q_count,
    pall, sall, sidx,
    own, pan, sown, dens, relay, pcode, scode,
    local_sem, plane_send, plane_recv, far_send, far_recv, c_send, c_recv, g_send, g_recv, s_send, s_recv, z_send, z_recv,
):
    row = lax.axis_index("row")
    col = lax.axis_index("col")
    y, x = row // 4, row % 4
    z, k = col // 2, col % 2

    load_own = pltpu.make_async_copy(coeffs, own, local_sem.at[0])
    load_s = pltpu.make_async_copy(sblk, sown, local_sem.at[1])
    load_own.start()
    load_s.start()

    barrier = pltpu.get_barrier_semaphore()
    for j in range(1, 16):
        pl.semaphore_signal(barrier, inc=1, device_id=(row, (col + j) % 16), device_id_type=MESH)
        pl.semaphore_signal(barrier, inc=1, device_id=((row + j) % 16, col), device_id_type=MESH)

    lane = lax.broadcasted_iota(jnp.int32, (8, B), 1)
    sub = lax.broadcasted_iota(jnp.int32, (8, B), 0)
    pc = jnp.full((8, B), -1, jnp.int32)
    qc = jnp.full((8, B), -100, jnp.int32)
    sc = jnp.full((8, B), -1, jnp.int32)
    p_live = jnp.full((8, B), p_count[0], jnp.int32)
    q_live = jnp.full((8, B), q_count[0], jnp.int32)
    s_live = jnp.full((8, B), s_count[0], jnp.int32)
    for i in range(8):
        pc = jnp.where((lane // 8 == i) & (p_live > i), jnp.full((8, B), p_slots[i], jnp.int32), pc)
        qc = jnp.where(
            (lane % 8 == i) & (lane < 64) & (q_live > i), jnp.full((8, B), q_slots[i], jnp.int32), qc
        )
        sc = jnp.where((sub == i) & (s_live > i), jnp.full((8, B), s_slots[i], jnp.int32), sc)
    pcode[col] = pc
    scode[row] = sc

    load_own.wait()
    load_s.wait()

    pl.semaphore_wait(barrier, 30)

    def slice_of(at):
        return own.at[pl.ds(4 * k, 4), :, pl.ds(pl.multiple_of(at * B, B), B)]

    class Piece:
        def __init__(self, e, table):
            self.shift = lookup(table, z)
            self.e, self.moves = e, 0 not in table
            self.peer = row ^ self.shift
            self.panel = row ^ self.shift

        def copy_in_plane(self):
            return pltpu.make_async_remote_copy(
                src_ref=slice_of(self.peer), dst_ref=relay.at[self.e],
                send_sem=plane_send.at[self.e], recv_sem=plane_recv.at[self.e],
                device_id=(self.peer, col), device_id_type=MESH,
            )

        def moved(self, act):
            if self.moves:
                act()
            else:
                pl.when(self.shift != 0)(act)

        def stays(self, act):
            if not self.moves:
                pl.when(self.shift == 0)(act)

        def far(self, src):
            return pltpu.make_async_remote_copy(
                src_ref=src, dst_ref=pan.at[row, pl.ds(4 * k, 4)],
                send_sem=far_send.at[self.e], recv_sem=far_recv.at[k],
                device_id=(row, self.panel), device_id_type=MESH,
            )

        def near(self, src):
            return pltpu.make_async_copy(src, pan.at[row, pl.ds(4 * k, 4)], far_recv.at[k])

        def hand_on(self, src):
            @pl.when(self.panel == col)
            def _():
                self.near(src).start()

            @pl.when(self.panel != col)
            def _():
                self.far(src).start()

    pieces = [Piece(0, FIRST), Piece(1, SECOND)]
    for piece in pieces:
        piece.moved(lambda piece=piece: piece.copy_in_plane().start())
        piece.stays(lambda piece=piece: piece.hand_on(slice_of(row)))

    place = (y, x, col)
    panel = PlaneGather(pan, pan.at[row], c_send, c_recv, place)
    inter = PlaneGather(sall, sown, s_send, s_recv, place)
    keep_s = pltpu.make_async_copy(sown, sall.at[row], local_sem.at[2])
    keep_s.start()

    for piece in pieces:

        def pass_along(piece=piece):
            piece.copy_in_plane().wait_recv()
            piece.hand_on(relay.at[piece.e])

        piece.moved(pass_along)

    for half in range(2):
        inter.first(half)
    codes = []
    for j in range(1, 16):
        link = Link(g_send, g_recv, 2 * j - 2)
        link.start(pcode.at[col], pcode.at[col], (row, (col + j) % 16))
        codes.append(link)
        link = Link(g_send, g_recv, 2 * j - 1)
        link.start(scode.at[row], scode.at[row], ((row + j) % 16, col))
        codes.append(link)
    for half in range(2):
        inter.second(half, 0)

    my_plane = lookup(PLANE, row ^ col)
    for half in range(2):
        landing = pan.at[row, pl.ds(4 * half, 4)]
        by_me = (my_plane == z) & (k == half)

        @pl.when(by_me)
        def _(landing=landing, half=half):
            pltpu.make_async_copy(landing, landing, far_recv.at[half]).wait()

        @pl.when(jnp.logical_not(by_me))
        def _(landing=landing, half=half):
            pltpu.make_async_remote_copy(
                src_ref=landing, dst_ref=landing, send_sem=far_send.at[0], recv_sem=far_recv.at[half],
                device_id=(row, col + 1 - 2 * k), device_id_type=MESH,
            ).wait_recv()

        panel.first(half)
        panel.second(half, 0)
    for side in range(2):
        for half in range(2):
            inter.relay_first(half, side)
    for side in range(2):
        for half in range(2):
            panel.relay_first(half, side)
            panel.second(half, 1 + side)
    for half in range(2):
        panel.far_first(half)
        panel.second(half, 3)

    for j in range(1, 16):
        codes[2 * j - 2].arrived(pcode.at[(col - j + 16) % 16], (row, (col - j + 16) % 16))
        codes[2 * j - 1].arrived(scode.at[(row - j + 16) % 16], ((row - j + 16) % 16, col))
    pcs, scs = pcode[...], scode[...]
    q = qc[None]
    match = ((pcs >> 3) == (q >> 3)) & ((scs >> 3) == (pcs & 7)) & ((scs & 7) == (q & 7))
    match = match & (pcs >= 0) & (scs >= 0) & (q >= 0)
    found = jnp.where(match, lax.broadcasted_iota(jnp.int32, (16, 8, B), 1) + 1, 0)
    found = jnp.sum(found, axis=1)
    source = lax.broadcasted_iota(jnp.int32, (B, B), 0)
    target = lax.broadcasted_iota(jnp.int32, (B, B), 1)
    counted = (target == 64 + (source >> 3)) | (target == 72)
    counts = jnp.dot(
        (found > 0).astype(jnp.float32), counted.astype(jnp.float32), preferred_element_type=jnp.float32
    )
    sidx[...] = jnp.where(lax.broadcasted_iota(jnp.int32, (16, B), 1) < 64, found, counts.astype(jnp.int32))

    for half in range(2):
        inter.far_first(half)
    for j in range(4):
        for side in range(2):
            for half in range(2):
                panel.relay_second(half, j, side)
    for j in range(4):
        for half in range(2):
            panel.far_second(half, j)

    for j in range(1, 4):
        for half in range(2):
            inter.second(half, j)

    for s in range(8):
        a = p_slots[s] >> 3
        b = p_slots[s] & 7
        left = own[a]
        right = jnp.concatenate([pan[i, b] for i in range(16)], axis=1)
        raw = lax.dot_general(left, right, (((1,), (1,)), ((), ())), preferred_element_type=jnp.float32)
        raw = jnp.where(jnp.full((B, B), p_count[0], jnp.int32) > s, raw, 0.0)
        dens[s] = raw.astype(jnp.bfloat16)

    sibling = (row, col + 1 - 2 * k)
    up = (row, (col + 2) % 16)
    down = (row, (col + 14) % 16)
    half_rows = dens.shape[0] // 2
    ring = [Link(z_send, z_recv, m) for m in range(30)]

    def tile(at, chunk):
        return pall.at[at, pl.ds(chunk * half_rows, half_rows)]

    def number(way, distance, chunk):
        return 7 * way + (2 * (distance - 1) + chunk if distance < 4 else 6)

    for chunk in range(2):
        src = dens.at[pl.ds(chunk * half_rows, half_rows)]
        ring[number(0, 1, chunk)].start(src, tile(col, chunk), up)
        ring[number(1, 1, chunk)].start(src, tile(col, chunk), down)
    for chunk in range(2):
        ring[14 + chunk].start(dens.at[pl.ds(chunk * half_rows, half_rows)], tile(col, chunk), sibling)
    keep_p = pltpu.make_async_copy(dens, pall.at[col], local_sem.at[3])
    keep_p.start()

    def pass_on(way, distance, chunk):
        at = (col + 16 - 2 * distance) % 16 if way == 0 else (col + 2 * distance) % 16
        here = tile(at, chunk)
        me = number(way, distance, chunk)
        ring[me].arrived(here, down if way == 0 else up)
        if distance < 3 or (distance == 3 and chunk == way):
            ring[number(way, distance + 1, chunk)].start(here, here, up if way == 0 else down)
        ring[16 + me].start(here, here, sibling)

    def across(me, at, chunk):
        ring[me].arrived(tile(at, chunk), sibling)

    arrivals = [(d, c) for d in (1, 2, 3) for c in range(2)]
    relays = [(j, side) for j in range(4) for side in range(2)]
    for n in range(8):
        if n < 6:
            for way in range(2):
                pass_on(way, *arrivals[n])
        j, side = relays[n]
        for half in range(2):
            inter.relay_second(half, j, side)
    for way in range(2):
        pass_on(way, 4, way)
    for j in range(4):
        for half in range(2):
            inter.far_second(half, j)
    other = col + 1 - 2 * k
    for chunk in range(2):
        across(14 + chunk, other, chunk)
    for way in range(2):
        for distance in (1, 2, 3):
            for chunk in range(2):
                at = (other + 16 - 2 * distance) % 16 if way == 0 else (other + 2 * distance) % 16
                across(16 + number(way, distance, chunk), at, chunk)
        across(16 + number(way, 4, way), (other + 8) % 16, way)

    keep_s.wait()
    keep_p.wait()
    panel.finish()
    inter.finish()
    for link in codes + ring:
        link.sent.wait_send()
    for piece in pieces:
        piece.moved(lambda piece=piece: piece.copy_in_plane().wait_send())

        @pl.when(piece.panel != col)
        def _(piece=piece):
            piece.far(relay.at[piece.e]).wait_send()


def product_kernel(sidx, pall, sall, out, dens, todo, pbuf, sbuf, count, sem, sem_p, sem_s):
    depth = pbuf.shape[0]
    col = lax.axis_index("col")
    keep = pltpu.make_async_copy(pall.at[col], dens, sem.at[0])
    keep.start()
    count[0] = 0

    def copies(i, code):
        t, p, s = code // 1024, code // 128 % 8, code % 16
        at = i % depth
        return (
            pltpu.make_async_copy(pall.at[t, p], pbuf.at[at], sem_p.at[at]),
            pltpu.make_async_copy(sall.at[t, s], sbuf.at[at], sem_s.at[at]),
        )

    def begin(i, code):
        for copy in copies(i, code):
            copy.start()

    def tile(t, _):
        @pl.when(sidx[t, 72] > 0)
        def _():
            def slot(p, _):
                @pl.when(sidx[t, 64 + p] > 0)
                def _():
                    def pair(q, _):
                        v = sidx[t, 8 * p + q]

                        @pl.when(v > 0)
                        def _():
                            n = count[0]
                            code = t * 1024 + p * 128 + q * 16 + v - 1
                            todo[n] = code
                            count[0] = n + 1

                            @pl.when(n < depth)
                            def _():
                                begin(n, code)

                        return 0

                    lax.fori_loop(0, 8, pair, 0)

                return 0

            lax.fori_loop(0, 8, slot, 0)

        return 0

    lax.fori_loop(0, 16, tile, 0)
    n = count[0]
    out[...] = jnp.zeros_like(out)

    def work(i, _):
        code = todo[i]
        for copy in copies(i, code):
            copy.wait()
        at = i % depth
        q = code // 16 % 8
        out[q] += jnp.dot(pbuf[at], sbuf[at], preferred_element_type=jnp.float32)

        @pl.when(i + depth < n)
        def _():
            begin(i + depth, todo[i + depth])

        return 0

    lax.fori_loop(0, n, work, 0)
    keep.wait()


def on_device(coeffs, p_slots, p_count, s_blocks, s_slots, s_count, q_slots, q_count):
    rows, orbitals = coeffs.shape
    n = 16
    smem = pl.BlockSpec(memory_space=pltpu.SMEM)
    vmem = pl.BlockSpec(memory_space=pltpu.VMEM)
    anyspace = pl.BlockSpec(memory_space=pl.ANY)
    gathered = jax.ShapeDtypeStruct((n, rows // B, B, B), jnp.bfloat16)
    dma = pltpu.SemaphoreType.DMA
    pall, sall, sidx = pl.pallas_call(
        gather_kernel,
        out_shape=(
            gathered, gathered, jax.ShapeDtypeStruct((n, B), jnp.int32),
        ),
        in_specs=[anyspace, anyspace] + [smem] * 6,
        out_specs=(anyspace, anyspace, vmem),
        scratch_shapes=[
            pltpu.VMEM((rows // B, B, orbitals), jnp.bfloat16),
            pltpu.VMEM((n, rows // B, B, B), jnp.bfloat16),
            pltpu.VMEM((rows // B, B, B), jnp.bfloat16),
            pltpu.VMEM((rows // B, B, B), jnp.bfloat16),
            pltpu.VMEM((2, rows // B // 2, B, B), jnp.bfloat16),
            pltpu.VMEM((n, 8, B), jnp.int32),
            pltpu.VMEM((n, 8, B), jnp.int32),
            dma((4,)), dma((2,)), dma((2,)), dma((2,)), dma((2,)),
            dma((40,)), dma((40,)), dma((30,)), dma((30,)), dma((40,)), dma((40,)), dma((30,)), dma((30,)),
        ],
        compiler_params=pltpu.CompilerParams(collective_id=0, has_side_effects=True),
        name="gather",
    )(
        coeffs.reshape(rows // B, B, orbitals), s_blocks.reshape(rows // B, B, B), p_slots.reshape(8), p_count.reshape(1), s_slots.reshape(8),
        s_count.reshape(1), q_slots.reshape(8), q_count.reshape(1),
    )
    depth = 32
    product, dens = pl.pallas_call(
        product_kernel,
        out_shape=(
            jax.ShapeDtypeStruct((8, B, B), jnp.float32), jax.ShapeDtypeStruct((8, B, B), jnp.bfloat16)
        ),
        in_specs=[smem, anyspace, anyspace],
        out_specs=(vmem, vmem),
        scratch_shapes=[
            pltpu.SMEM((1024,), jnp.int32),
            pltpu.VMEM((depth, B, B), jnp.bfloat16),
            pltpu.VMEM((depth, B, B), jnp.bfloat16),
            pltpu.SMEM((1,), jnp.int32),
            dma((1,)), dma((depth,)), dma((depth,)),
        ],
        name="product",
    )(sidx, pall, sall)
    return dens.reshape(1, 1, 8, B, B), product.reshape(1, 1, 8, B, B)


def solution(mesh):
    return jax.shard_map(
        on_device,
        mesh=mesh,
        in_specs=(
            P("row", None),
            P("row", "col", None),
            P("row", "col"),
            P("row", "col", None, None, None),
            P("row", "col", None),
            P("row", "col"),
            P("row", "col", None),
            P("row", "col"),
        ),
        out_specs=(P("row", "col", None, None, None), P("row", "col", None, None, None)),
        check_vma=False,
    )
```

```python
import functools

import jax
import jax.numpy as jnp
from jax import lax
from jax.experimental import pallas as pl
from jax.experimental.pallas import tpu as pltpu
from jax.sharding import PartitionSpec as P

MESH = pl.DeviceIdType.MESH
B = 128
FIRST = (8, 11, 6, 9, 14, 7, 10, 5)
SECOND = (2, 1, 12, 3, 4, 13, 0, 15)
PLANE = tuple((FIRST if i in FIRST else SECOND).index(i) for i in range(16))


def lookup(table, at):
    value = 0
    for base in range(0, len(table), 4):
        packed = sum(table[base + i] << (4 * i) for i in range(4))
        inside = (at // 4 == base // 4).astype(jnp.int32)
        value = value + inside * ((packed // (1 << (4 * (at % 4)))) % 16)
    return value


class Link:
    def __init__(self, send, recv, at):
        self.send, self.recv, self.at = send, recv, at

    def start(self, src, dst, device):
        pltpu.make_async_remote_copy(
            src_ref=src, dst_ref=dst, send_sem=self.send.at[0], recv_sem=self.recv.at[self.at],
            device_id=device, device_id_type=MESH,
        ).start()

    def arrived(self, landing, device):
        pltpu.make_async_remote_copy(
            src_ref=landing, dst_ref=landing, send_sem=self.send.at[0], recv_sem=self.recv.at[self.at],
            device_id=device, device_id_type=MESH,
        ).wait_recv()


def all_sent(send, whole, device):
    pltpu.make_async_remote_copy(
        src_ref=whole, dst_ref=whole, send_sem=send.at[0], recv_sem=send.at[0], device_id=device, device_id_type=MESH
    ).wait_send()


class PlaneGather:
    def __init__(self, buf, own, send, recv, place, streams):
        self.buf, self.own = buf, own
        self.y, self.x, self.col = place
        self.size = own.shape[0] // streams
        self.links = [Link(send, recv, m) for m in range(20 * streams)]

    def index(self, stream, du, dv):
        if stream % 2 == 0:
            return 4 * ((self.y + dv + 4) % 4) + (self.x + du + 4) % 4
        return 4 * ((self.y + du + 4) % 4) + (self.x + dv + 4) % 4

    def device(self, stream, du, dv):
        return (self.index(stream, du, dv), self.col)

    def span(self, stream, part):
        base = (stream % 2) * self.own.shape[0] // 2 + (stream // 2) * self.size
        if part is None:
            return pl.ds(base, self.size)
        return pl.ds(base + part * (self.size // 2), self.size // 2)

    def block(self, stream, du, dv, part=None):
        return self.buf.at[self.index(stream, du, dv), self.span(stream, part)]

    def link(self, stream, number):
        return self.links[20 * stream + number]

    def first(self, stream):
        src = self.own.at[self.span(stream, None)]
        dst = self.block(stream, 0, 0)
        self.link(stream, 0).start(src, dst, self.device(stream, 1, 0))
        self.link(stream, 1).start(src, dst, self.device(stream, -1, 0))

    def relay_first(self, stream, side):
        du = -1 if side == 0 else 1
        self.link(stream, side).arrived(self.block(stream, du, 0), self.device(stream, du, 0))
        part = self.block(stream, du, 0, side)
        self.link(stream, 2 + side).start(part, part, self.device(stream, -du, 0))

    def far_first(self, stream):
        for side in range(2):
            part = self.block(stream, 2, 0, side)
            self.link(stream, 2 + side).arrived(part, self.device(stream, -1 if side == 0 else 1, 0))

    def second(self, stream, j):
        du = (0, -1, 1, 2)[j]
        dst = self.block(stream, du, 0)
        src = self.own.at[self.span(stream, None)] if j == 0 else dst
        self.link(stream, 4 + 4 * j).start(src, dst, self.device(stream, 0, 1))
        self.link(stream, 5 + 4 * j).start(src, dst, self.device(stream, 0, -1))

    def relay_second(self, stream, j, side):
        du = (0, -1, 1, 2)[j]
        dv = -1 if side == 0 else 1
        number = 4 + 4 * j + side
        self.link(stream, number).arrived(self.block(stream, du, dv), self.device(stream, 0, dv))
        part = self.block(stream, du, dv, side)
        self.link(stream, number + 2).start(part, part, self.device(stream, 0, -dv))

    def far_second(self, stream, j):
        du = (0, -1, 1, 2)[j]
        for side in range(2):
            part = self.block(stream, du, 2, side)
            self.link(stream, 6 + 4 * j + side).arrived(part, self.device(stream, 0, -1 if side == 0 else 1))

    def finish(self):
        all_sent(self.links[0].send, self.buf.at[pl.ds(0, 15)], self.device(0, 1, 0))


def gather_kernel(
    coeffs, sblk, p_slots, p_count, s_slots, s_count, q_slots, q_count,
    pall, sall, sidx,
    own, pan, sown, dens, held, relay, code_v, sidx_v,
    local_sem, plane_send, plane_recv, far_send, far_recv, c_send, c_recv, g_send, g_recv, s_send, s_recv, z_send, z_recv,
    x_send, x_recv, keep_sem,
):
    row = lax.axis_index("row")
    col = lax.axis_index("col")
    pcode, scode = code_v.at[pl.ds(0, 16)], code_v.at[pl.ds(16, 16)]
    codes_sent = code_v.at[pl.ds(0, 30)]
    y, x = row // 4, row % 4
    z, k = col // 2, col % 2

    load_own = pltpu.make_async_copy(coeffs, own, local_sem.at[0])
    load_s = pltpu.make_async_copy(sblk, sown, local_sem.at[1])
    load_own.start()
    load_s.start()

    barrier = pltpu.get_barrier_semaphore()
    for j in range(1, 16):
        pl.semaphore_signal(barrier, inc=1, device_id=(row, (col + j) % 16), device_id_type=MESH)
        pl.semaphore_signal(barrier, inc=1, device_id=((row + j) % 16, col), device_id_type=MESH)

    lane = lax.broadcasted_iota(jnp.int32, (8, B), 1)
    sub = lax.broadcasted_iota(jnp.int32, (8, B), 0)
    pc = jnp.full((8, B), -1, jnp.int32)
    qc = jnp.full((8, B), -100, jnp.int32)
    sc = jnp.full((8, B), -1, jnp.int32)
    p_live = jnp.full((8, B), p_count[0], jnp.int32)
    q_live = jnp.full((8, B), q_count[0], jnp.int32)
    s_live = jnp.full((8, B), s_count[0], jnp.int32)
    for i in range(8):
        pc = jnp.where((lane // 8 == i) & (p_live > i), jnp.full((8, B), p_slots[i], jnp.int32), pc)
        qc = jnp.where(
            (lane % 8 == i) & (lane < 64) & (q_live > i), jnp.full((8, B), q_slots[i], jnp.int32), qc
        )
        sc = jnp.where((sub == i) & (s_live > i), jnp.full((8, B), s_slots[i], jnp.int32), sc)
    pcode[col] = pc
    scode[row] = sc

    load_own.wait()
    load_s.wait()

    pl.semaphore_wait(barrier, 30)

    def slice_of(at, chunk):
        return own.at[4 * k + chunk, :, pl.ds(pl.multiple_of(at * B, B), B)]

    class Piece:
        def __init__(self, e, table):
            self.shift = lookup(table, z)
            self.e, self.moves = e, 0 not in table
            self.peer = row ^ self.shift

        def copy_in_plane(self, chunk):
            return pltpu.make_async_remote_copy(
                src_ref=slice_of(self.peer, chunk), dst_ref=relay.at[self.e, chunk],
                send_sem=plane_send.at[self.e, chunk], recv_sem=plane_recv.at[self.e, chunk],
                device_id=(self.peer, col), device_id_type=MESH,
            )

        def moved(self, act):
            if self.moves:
                act()
            else:
                pl.when(self.shift != 0)(act)

        def stays(self, act):
            if not self.moves:
                pl.when(self.shift == 0)(act)

        def far(self, src, chunk):
            return pltpu.make_async_remote_copy(
                src_ref=src, dst_ref=pan.at[row, 4 * k + chunk],
                send_sem=far_send.at[self.e, chunk], recv_sem=far_recv.at[k, chunk],
                device_id=(row, self.peer), device_id_type=MESH,
            )

        def hand_on(self, src, chunk):
            @pl.when(self.peer == col)
            def _():
                pltpu.make_async_copy(src, pan.at[row, 4 * k + chunk], far_recv.at[k, chunk]).start()

            @pl.when(self.peer != col)
            def _():
                self.far(src, chunk).start()

    pieces = [Piece(0, FIRST), Piece(1, SECOND)]
    for chunk in range(4):
        for piece in pieces:
            piece.moved(lambda piece=piece, chunk=chunk: piece.copy_in_plane(chunk).start())
            piece.stays(lambda piece=piece, chunk=chunk: piece.hand_on(slice_of(row, chunk), chunk))

    place = (y, x, col)
    panel = PlaneGather(pan, pan.at[row], c_send, c_recv, place, 4)
    inter = PlaneGather(sall, sown, s_send, s_recv, place, 2)
    keep_s = pltpu.make_async_copy(sown, sall.at[row], local_sem.at[2])
    keep_s.start()

    for chunk in range(4):
        for piece in pieces:

            def pass_along(piece=piece, chunk=chunk):
                piece.copy_in_plane(chunk).wait_recv()
                piece.hand_on(relay.at[piece.e, chunk], chunk)

            piece.moved(pass_along)

    for half in range(2):
        inter.first(half)
    codes = [Link(g_send, g_recv, m) for m in range(8)]

    def code_step(step, act):
        size = 1 << step
        for dim, (ref, me) in enumerate(((pcode, col), (scode, row))):
            mine = me // size * size
            other = me ^ size
            device = (row, other) if dim == 0 else (other, col)
            if act == "start":
                here = ref.at[pl.ds(mine, size)]
                codes[2 * step + dim].start(here, here, device)
            else:
                codes[2 * step + dim].arrived(ref.at[pl.ds(mine ^ size, size)], device)

    code_step(0, "start")

    my_plane = lookup(PLANE, row ^ col)

    def scattered(half, chunk):
        by_me = (my_plane == z) & (k == half)
        landing = pan.at[row, 4 * half + chunk]

        @pl.when(by_me)
        def _():
            pltpu.make_async_copy(landing, landing, far_recv.at[half, chunk]).wait()

        @pl.when(jnp.logical_not(by_me))
        def _():
            pltpu.make_async_remote_copy(
                src_ref=landing, dst_ref=landing, send_sem=far_send.at[0, chunk],
                recv_sem=far_recv.at[half, chunk],
                device_id=(row, col + 1 - 2 * k), device_id_type=MESH,
            ).wait_recv()

    sibling = (row, col + 1 - 2 * k)
    up = (row, (col + 2) % 16)
    down = (row, (col + 14) % 16)
    chunks = 4
    size = dens.shape[0] // chunks
    ring = [Link(z_send, z_recv, m) for m in range(7 * chunks)]
    over = [Link(x_send, x_recv, m) for m in range(8)]

    def number(way, distance, chunk):
        return 7 * chunks // 2 * way + (
            chunks * (distance - 1) + chunk if distance < 4 else 3 * chunks + chunk % (chunks // 2)
        )

    def z_of(way, distance):
        return (z + 8 - distance) % 8 if way == 0 else (z + distance) % 8

    def part(ref, chunk):
        return ref.at[pl.ds(chunk * size, size)]

    def ring_start():
        for chunk in range(chunks):
            for way in range(2):
                ring[number(way, 1, chunk)].start(
                    part(dens, chunk), part(held.at[z], chunk), up if way == 0 else down
                )
        over[0].start(dens, pall.at[col], sibling)
        keep(0).start()

    def keep(slot):
        if slot == 0:
            return pltpu.make_async_copy(dens, pall.at[col], keep_sem.at[0])
        at = z_of(0 if slot < 5 else 1, slot if slot < 5 else slot - 4)
        return pltpu.make_async_copy(held.at[at], pall.at[2 * at + k], keep_sem.at[slot])

    def goes_on(way, distance, chunk):
        return distance < 3 or (distance == 3 and (chunk < chunks // 2) == (way == 0))

    def pass_on(way, distance, chunk):
        here = part(held.at[z_of(way, distance)], chunk)
        ring[number(way, distance, chunk)].arrived(here, down if way == 0 else up)
        if goes_on(way, distance, chunk):
            ring[number(way, distance + 1, chunk)].start(here, here, up if way == 0 else down)
        if distance < 4 and chunk == chunks - 1:
            done(distance if way == 0 else 4 + distance)

    def done(slot):
        at = z_of(0 if slot < 5 else 1, slot if slot < 5 else slot - 4)
        keep(slot).start()
        over[slot].start(held.at[at], pall.at[2 * at + k], sibling)

    def ring_step(distance, chunk):
        for way in range(2):
            if distance < 4 or (chunk < chunks // 2) == (way == 0):
                pass_on(way, distance, chunk)

    steps = [(d, c) for d in (1, 2, 3) for c in range(chunks)] + [
        (4, c) for pair in range(chunks // 2) for c in (pair, pair + chunks // 2)
    ]

    def ring_end():
        for slot in range(8):
            at = z if slot == 0 else z_of(0 if slot < 5 else 1, slot if slot < 5 else slot - 4)
            over[slot].arrived(pall.at[2 * at + 1 - k], sibling)
        for slot in range(8):
            keep(slot).wait()

    def meet():
        code_step(3, "arrived")
        pcs, scs = pcode[...], scode[...]
        q = qc[None]
        match = ((pcs >> 3) == (q >> 3)) & ((scs >> 3) == (pcs & 7)) & ((scs & 7) == (q & 7))
        match = match & (pcs >= 0) & (scs >= 0) & (q >= 0)
        found = jnp.where(match, lax.broadcasted_iota(jnp.int32, (16, 8, B), 1) + 1, 0)
        found = jnp.sum(found, axis=1)
        source = lax.broadcasted_iota(jnp.int32, (B, B), 0)
        target = lax.broadcasted_iota(jnp.int32, (B, B), 1)
        counted = (target == 64 + (source >> 3)) | (target == 72)
        counts = jnp.dot(
            (found > 0).astype(jnp.float32), counted.astype(jnp.float32), preferred_element_type=jnp.float32
        )
        sidx_v[...] = jnp.where(lax.broadcasted_iota(jnp.int32, (16, B), 1) < 64, found, counts.astype(jnp.int32))
        pltpu.make_async_copy(sidx_v, sidx, local_sem.at[3]).start()

    def density():
        for s in range(8):
            a = p_slots[s] >> 3
            b = p_slots[s] & 7
            left = own[a]
            right = jnp.concatenate([pan[i, b] for i in range(16)], axis=1)
            raw = lax.dot_general(left, right, (((1,), (1,)), ((), ())), preferred_element_type=jnp.float32)
            raw = jnp.where(jnp.full((B, B), p_count[0], jnp.int32) > s, raw, 0.0)
            dens[s] = raw.astype(jnp.bfloat16)

    def inter_sends():
        for j in range(4):
            for half in range(2):
                inter.second(half, j)

    relays = [(j, side) for j in range(4) for side in range(2)]

    def inter_step(j, side):
        for half in range(2):
            inter.relay_second(half, j, side)

    def turn(core):
        for wave in range(2):
            for half in range(2):
                for chunk in range(2 * wave, 2 * wave + 2):
                    scattered(half, chunk)
                panel.first(2 * wave + half)
                panel.second(2 * wave + half, 0)
            if wave == 0:
                for side in range(2):
                    for half in range(2):
                        inter.relay_first(half, side)
                code_step(0, "arrived")
                code_step(1, "start")
            for side in range(2):
                for half in range(2):
                    panel.relay_first(2 * wave + half, side)
                    panel.second(2 * wave + half, 1 + side)
            code_step(1 + wave, "arrived")
            code_step(2 + wave, "start")
        for stream in range(4):
            panel.far_first(stream)
            panel.second(stream, 3)
        meet()
        for half in range(2):
            inter.far_first(half)
        for wave in range(2):
            for j in range(4):
                for side in range(2):
                    for half in range(2):
                        panel.relay_second(2 * wave + half, j, side)
        for j in range(4):
            for stream in range(4):
                panel.far_second(stream, j)
        inter_sends()
        density()
        ring_start()
        if True:
            for n, step in enumerate(steps):
                ring_step(*step)
                if 2 <= n < 2 + len(relays):
                    inter_step(*relays[n - 2])
        done(4)
        for j in range(4):
            for half in range(2):
                inter.far_second(half, j)
        ring_end()
        keep_s.wait()
        pltpu.make_async_copy(sidx_v, sidx, local_sem.at[3]).wait()
        panel.finish()
        inter.finish()
        all_sent(g_send, codes_sent, sibling)
        all_sent(z_send, held.at[pl.ds(0, 7)], sibling)
        all_sent(x_send, held, sibling)

    turn(2)

    for chunk in range(4):
        for piece in pieces:
            piece.moved(lambda piece=piece, chunk=chunk: piece.copy_in_plane(chunk).wait_send())

            @pl.when(piece.peer != col)
            def _(piece=piece, chunk=chunk):
                piece.far(relay.at[piece.e, chunk], chunk).wait_send()


def product_kernel(sidx, pall, sall, out, dens, todo, pbuf, sbuf, count, sem, sem_p, sem_s):
    depth = pbuf.shape[0]
    col = lax.axis_index("col")
    keep = pltpu.make_async_copy(pall.at[col], dens, sem.at[0])
    keep.start()
    count[0] = 0

    def copies(i, code):
        t, p, s = code // 1024, code // 128 % 8, code % 16
        at = i % depth
        return (
            pltpu.make_async_copy(pall.at[t, p], pbuf.at[at], sem_p.at[at]),
            pltpu.make_async_copy(sall.at[t, s], sbuf.at[at], sem_s.at[at]),
        )

    def begin(i, code):
        for copy in copies(i, code):
            copy.start()

    def tile(t, _):
        @pl.when(sidx[t, 72] > 0)
        def _():
            def slot(p, _):
                @pl.when(sidx[t, 64 + p] > 0)
                def _():
                    def pair(q, _):
                        v = sidx[t, 8 * p + q]

                        @pl.when(v > 0)
                        def _():
                            n = count[0]
                            code = t * 1024 + p * 128 + q * 16 + v - 1
                            todo[n] = code
                            count[0] = n + 1

                            @pl.when(n < depth)
                            def _():
                                begin(n, code)

                        return 0

                    lax.fori_loop(0, 8, pair, 0)

                return 0

            lax.fori_loop(0, 8, slot, 0)

        return 0

    lax.fori_loop(0, 16, tile, 0)
    n = count[0]
    out[...] = jnp.zeros_like(out)

    def work(i, _):
        code = todo[i]
        for copy in copies(i, code):
            copy.wait()
        at = i % depth
        q = code // 16 % 8
        out[q] += jnp.dot(pbuf[at], sbuf[at], preferred_element_type=jnp.float32)

        @pl.when(i + depth < n)
        def _():
            begin(i + depth, todo[i + depth])

        return 0

    lax.fori_loop(0, n, work, 0)
    keep.wait()


def on_device(coeffs, p_slots, p_count, s_blocks, s_slots, s_count, q_slots, q_count):
    rows, orbitals = coeffs.shape
    n = 16
    smem = pl.BlockSpec(memory_space=pltpu.SMEM)
    vmem = pl.BlockSpec(memory_space=pltpu.VMEM)
    anyspace = pl.BlockSpec(memory_space=pl.ANY)
    gathered = jax.ShapeDtypeStruct((n, rows // B, B, B), jnp.bfloat16)
    dma = pltpu.SemaphoreType.DMA
    pall, sall, sidx = pl.pallas_call(
        gather_kernel,
        out_shape=(
            gathered, gathered, jax.ShapeDtypeStruct((n, B), jnp.int32),
        ),
        in_specs=[anyspace, anyspace] + [smem] * 6,
        out_specs=(anyspace, anyspace, anyspace),
        scratch_shapes=[
            pltpu.VMEM((rows // B, B, orbitals), jnp.bfloat16),
            pltpu.VMEM((n, rows // B, B, B), jnp.bfloat16),
            pltpu.VMEM((rows // B, B, B), jnp.bfloat16),
            pltpu.VMEM((rows // B, B, B), jnp.bfloat16),
            pltpu.VMEM((8, rows // B, B, B), jnp.bfloat16),
            pltpu.VMEM((2, rows // B // 2, B, B), jnp.bfloat16),
            pltpu.VMEM((2 * n, 8, B), jnp.int32),
            pltpu.VMEM((n, B), jnp.int32),
            dma((4,)), dma((2, 4)), dma((2, 4)), dma((2, 4)), dma((2, 4)),
            dma((1,)), dma((80,)), dma((1,)), dma((8,)), dma((1,)), dma((40,)), dma((1,)), dma((28,)),
            dma((1,)), dma((8,)), dma((8,)),
        ],
        compiler_params=pltpu.CompilerParams(collective_id=0, has_side_effects=True),
        name="gather",
    )(
        coeffs.reshape(rows // B, B, orbitals), s_blocks.reshape(rows // B, B, B), p_slots.reshape(8), p_count.reshape(1), s_slots.reshape(8),
        s_count.reshape(1), q_slots.reshape(8), q_count.reshape(1),
    )
    depth = 32
    product, dens = pl.pallas_call(
        product_kernel,
        out_shape=(
            jax.ShapeDtypeStruct((8, B, B), jnp.float32), jax.ShapeDtypeStruct((8, B, B), jnp.bfloat16)
        ),
        in_specs=[smem, anyspace, anyspace],
        out_specs=(vmem, vmem),
        scratch_shapes=[
            pltpu.SMEM((1024,), jnp.int32),
            pltpu.VMEM((depth, B, B), jnp.bfloat16),
            pltpu.VMEM((depth, B, B), jnp.bfloat16),
            pltpu.SMEM((1,), jnp.int32),
            dma((1,)), dma((depth,)), dma((depth,)),
        ],
        name="product",
    )(sidx, pall, sall)
    return dens.reshape(1, 1, 8, B, B), product.reshape(1, 1, 8, B, B)


def solution(mesh):
    return jax.shard_map(
        on_device,
        mesh=mesh,
        in_specs=(
            P("row", None),
            P("row", "col", None),
            P("row", "col"),
            P("row", "col", None, None, None),
            P("row", "col", None),
            P("row", "col"),
            P("row", "col", None),
            P("row", "col"),
        ),
        out_specs=(P("row", "col", None, None, None), P("row", "col", None, None, None)),
        check_vma=False,
    )
```

```python
import functools

import jax
import jax.numpy as jnp
from jax import lax
from jax.experimental import pallas as pl
from jax.experimental.pallas import tpu as pltpu
from jax.sharding import PartitionSpec as P

MESH = pl.DeviceIdType.MESH
B = 128
LISTED = 128
FIRST = (8, 11, 6, 9, 14, 7, 10, 5)
SECOND = (2, 1, 12, 3, 4, 13, 0, 15)
PLANE = tuple((FIRST if i in FIRST else SECOND).index(i) for i in range(16))


def lookup(table, at):
    value = 0
    for base in range(0, len(table), 4):
        packed = sum(table[base + i] << (4 * i) for i in range(4))
        inside = (at // 4 == base // 4).astype(jnp.int32)
        value = value + inside * ((packed // (1 << (4 * (at % 4)))) % 16)
    return value


class Link:
    def __init__(self, send, recv, at):
        self.send, self.recv, self.at = send, recv, at

    def start(self, src, dst, device):
        pltpu.make_async_remote_copy(
            src_ref=src, dst_ref=dst, send_sem=self.send.at[0], recv_sem=self.recv.at[self.at],
            device_id=device, device_id_type=MESH,
        ).start()

    def arrived(self, landing, device):
        pltpu.make_async_remote_copy(
            src_ref=landing, dst_ref=landing, send_sem=self.send.at[0], recv_sem=self.recv.at[self.at],
            device_id=device, device_id_type=MESH,
        ).wait_recv()


def all_sent(send, whole, device):
    pltpu.make_async_remote_copy(
        src_ref=whole, dst_ref=whole, send_sem=send.at[0], recv_sem=send.at[0], device_id=device, device_id_type=MESH
    ).wait_send()


class PlaneGather:
    def __init__(self, buf, own, send, recv, place, streams):
        self.buf, self.own = buf, own
        self.y, self.x, self.col = place
        self.size = own.shape[0] // streams
        self.links = [Link(send, recv, m) for m in range(20 * streams)]

    def index(self, stream, du, dv):
        if stream % 2 == 0:
            return 4 * ((self.y + dv + 4) % 4) + (self.x + du + 4) % 4
        return 4 * ((self.y + du + 4) % 4) + (self.x + dv + 4) % 4

    def device(self, stream, du, dv):
        return (self.index(stream, du, dv), self.col)

    def span(self, stream, part):
        base = (stream % 2) * self.own.shape[0] // 2 + (stream // 2) * self.size
        if part is None:
            return pl.ds(base, self.size)
        return pl.ds(base + part * (self.size // 2), self.size // 2)

    def block(self, stream, du, dv, part=None):
        return self.buf.at[self.index(stream, du, dv), self.span(stream, part)]

    def link(self, stream, number):
        return self.links[20 * stream + number]

    def first(self, stream):
        src = self.own.at[self.span(stream, None)]
        dst = self.block(stream, 0, 0)
        self.link(stream, 0).start(src, dst, self.device(stream, 1, 0))
        self.link(stream, 1).start(src, dst, self.device(stream, -1, 0))

    def relay_first(self, stream, side):
        du = -1 if side == 0 else 1
        self.link(stream, side).arrived(self.block(stream, du, 0), self.device(stream, du, 0))
        part = self.block(stream, du, 0, side)
        self.link(stream, 2 + side).start(part, part, self.device(stream, -du, 0))

    def far_first(self, stream):
        for side in range(2):
            part = self.block(stream, 2, 0, side)
            self.link(stream, 2 + side).arrived(part, self.device(stream, -1 if side == 0 else 1, 0))

    def second(self, stream, j):
        du = (0, -1, 1, 2)[j]
        dst = self.block(stream, du, 0)
        src = self.own.at[self.span(stream, None)] if j == 0 else dst
        self.link(stream, 4 + 4 * j).start(src, dst, self.device(stream, 0, 1))
        self.link(stream, 5 + 4 * j).start(src, dst, self.device(stream, 0, -1))

    def relay_second(self, stream, j, side):
        du = (0, -1, 1, 2)[j]
        dv = -1 if side == 0 else 1
        number = 4 + 4 * j + side
        self.link(stream, number).arrived(self.block(stream, du, dv), self.device(stream, 0, dv))
        part = self.block(stream, du, dv, side)
        self.link(stream, number + 2).start(part, part, self.device(stream, 0, -dv))

    def far_second(self, stream, j):
        du = (0, -1, 1, 2)[j]
        for side in range(2):
            part = self.block(stream, du, 2, side)
            self.link(stream, 6 + 4 * j + side).arrived(part, self.device(stream, 0, -1 if side == 0 else 1))

    def finish(self):
        all_sent(self.links[0].send, self.buf.at[pl.ds(0, 15)], self.device(0, 1, 0))


def gather_kernel(
    coeffs, sblk, p_slots, p_count, s_slots, s_count, q_slots, q_count,
    pall, sall, sidx,
    own, pan, sown, dens, held, relay, code_v, sidx_v,
    local_sem, plane_send, plane_recv, far_send, far_recv, c_send, c_recv, g_send, g_recv, s_send, s_recv, z_send, z_recv,
    x_send, x_recv, keep_sem,
):
    row = lax.axis_index("row")
    col = lax.axis_index("col")
    pcode, scode = code_v.at[pl.ds(0, 16)], code_v.at[pl.ds(16, 16)]
    codes_sent = code_v.at[pl.ds(0, 30)]
    y, x = row // 4, row % 4
    z, k = col // 2, col % 2

    load_own = pltpu.make_async_copy(coeffs, own, local_sem.at[0])
    load_s = pltpu.make_async_copy(sblk, sown, local_sem.at[1])
    load_own.start()
    load_s.start()

    barrier = pltpu.get_barrier_semaphore()
    for j in range(1, 16):
        pl.semaphore_signal(barrier, inc=1, device_id=(row, (col + j) % 16), device_id_type=MESH)
        pl.semaphore_signal(barrier, inc=1, device_id=((row + j) % 16, col), device_id_type=MESH)

    lane = lax.broadcasted_iota(jnp.int32, (8, B), 1)
    sub = lax.broadcasted_iota(jnp.int32, (8, B), 0)
    pc = jnp.full((8, B), -1, jnp.int32)
    qc = jnp.full((8, B), -100, jnp.int32)
    sc = jnp.full((8, B), -1, jnp.int32)
    p_live = jnp.full((8, B), p_count[0], jnp.int32)
    q_live = jnp.full((8, B), q_count[0], jnp.int32)
    s_live = jnp.full((8, B), s_count[0], jnp.int32)
    for i in range(8):
        pc = jnp.where((lane // 8 == i) & (p_live > i), jnp.full((8, B), p_slots[i], jnp.int32), pc)
        qc = jnp.where(
            (lane % 8 == i) & (lane < 64) & (q_live > i), jnp.full((8, B), q_slots[i], jnp.int32), qc
        )
        sc = jnp.where((sub == i) & (s_live > i), jnp.full((8, B), s_slots[i], jnp.int32), sc)
    pcode[col] = pc
    scode[row] = sc

    load_own.wait()
    load_s.wait()

    pl.semaphore_wait(barrier, 30)

    def slice_of(at, chunk):
        return own.at[4 * k + chunk, :, pl.ds(pl.multiple_of(at * B, B), B)]

    class Piece:
        def __init__(self, e, table):
            self.shift = lookup(table, z)
            self.e, self.moves = e, 0 not in table
            self.peer = row ^ self.shift

        def copy_in_plane(self, chunk):
            return pltpu.make_async_remote_copy(
                src_ref=slice_of(self.peer, chunk), dst_ref=relay.at[self.e, chunk],
                send_sem=plane_send.at[self.e, chunk], recv_sem=plane_recv.at[self.e, chunk],
                device_id=(self.peer, col), device_id_type=MESH,
            )

        def moved(self, act):
            if self.moves:
                act()
            else:
                pl.when(self.shift != 0)(act)

        def stays(self, act):
            if not self.moves:
                pl.when(self.shift == 0)(act)

        def far(self, src, chunk):
            return pltpu.make_async_remote_copy(
                src_ref=src, dst_ref=pan.at[row, 4 * k + chunk],
                send_sem=far_send.at[self.e, chunk], recv_sem=far_recv.at[k, chunk],
                device_id=(row, self.peer), device_id_type=MESH,
            )

        def hand_on(self, src, chunk):
            @pl.when(self.peer == col)
            def _():
                pltpu.make_async_copy(src, pan.at[row, 4 * k + chunk], far_recv.at[k, chunk]).start()

            @pl.when(self.peer != col)
            def _():
                self.far(src, chunk).start()

    pieces = [Piece(0, FIRST), Piece(1, SECOND)]
    for chunk in range(4):
        for piece in pieces:
            piece.moved(lambda piece=piece, chunk=chunk: piece.copy_in_plane(chunk).start())
            piece.stays(lambda piece=piece, chunk=chunk: piece.hand_on(slice_of(row, chunk), chunk))

    place = (y, x, col)
    panel = PlaneGather(pan, pan.at[row], c_send, c_recv, place, 4)
    inter = PlaneGather(sall, sown, s_send, s_recv, place, 2)
    keep_s = pltpu.make_async_copy(sown, sall.at[row], local_sem.at[2])
    keep_s.start()

    for chunk in range(4):
        for piece in pieces:

            def pass_along(piece=piece, chunk=chunk):
                piece.copy_in_plane(chunk).wait_recv()
                piece.hand_on(relay.at[piece.e, chunk], chunk)

            piece.moved(pass_along)

    for half in range(2):
        inter.first(half)
    codes = [Link(g_send, g_recv, m) for m in range(8)]

    def code_step(step, act):
        size = 1 << step
        for dim, (ref, me) in enumerate(((pcode, col), (scode, row))):
            mine = me // size * size
            other = me ^ size
            device = (row, other) if dim == 0 else (other, col)
            if act == "start":
                here = ref.at[pl.ds(mine, size)]
                codes[2 * step + dim].start(here, here, device)
            else:
                codes[2 * step + dim].arrived(ref.at[pl.ds(mine ^ size, size)], device)

    code_step(0, "start")

    my_plane = lookup(PLANE, row ^ col)

    def scattered(half, chunk):
        by_me = (my_plane == z) & (k == half)
        landing = pan.at[row, 4 * half + chunk]

        @pl.when(by_me)
        def _():
            pltpu.make_async_copy(landing, landing, far_recv.at[half, chunk]).wait()

        @pl.when(jnp.logical_not(by_me))
        def _():
            pltpu.make_async_remote_copy(
                src_ref=landing, dst_ref=landing, send_sem=far_send.at[0, chunk],
                recv_sem=far_recv.at[half, chunk],
                device_id=(row, col + 1 - 2 * k), device_id_type=MESH,
            ).wait_recv()

    sibling = (row, col + 1 - 2 * k)
    up = (row, (col + 2) % 16)
    down = (row, (col + 14) % 16)
    chunks = 4
    size = dens.shape[0] // chunks
    ring = [Link(z_send, z_recv, m) for m in range(7 * chunks)]
    over = [Link(x_send, x_recv, m) for m in range(8)]

    def number(way, distance, chunk):
        return 7 * chunks // 2 * way + (
            chunks * (distance - 1) + chunk if distance < 4 else 3 * chunks + chunk % (chunks // 2)
        )

    def z_of(way, distance):
        return (z + 8 - distance) % 8 if way == 0 else (z + distance) % 8

    def part(ref, chunk):
        return ref.at[pl.ds(chunk * size, size)]

    def ring_start():
        for chunk in range(chunks):
            for way in range(2):
                ring[number(way, 1, chunk)].start(
                    part(dens, chunk), part(held.at[z], chunk), up if way == 0 else down
                )
        over[0].start(dens, pall.at[col], sibling)
        keep(0).start()

    def keep(slot):
        if slot == 0:
            return pltpu.make_async_copy(dens, pall.at[col], keep_sem.at[0])
        at = z_of(0 if slot < 5 else 1, slot if slot < 5 else slot - 4)
        return pltpu.make_async_copy(held.at[at], pall.at[2 * at + k], keep_sem.at[slot])

    def goes_on(way, distance, chunk):
        return distance < 3 or (distance == 3 and (chunk < chunks // 2) == (way == 0))

    def pass_on(way, distance, chunk):
        here = part(held.at[z_of(way, distance)], chunk)
        ring[number(way, distance, chunk)].arrived(here, down if way == 0 else up)
        if goes_on(way, distance, chunk):
            ring[number(way, distance + 1, chunk)].start(here, here, up if way == 0 else down)
        if distance < 4 and chunk == chunks - 1:
            done(distance if way == 0 else 4 + distance)

    def done(slot):
        at = z_of(0 if slot < 5 else 1, slot if slot < 5 else slot - 4)
        keep(slot).start()
        over[slot].start(held.at[at], pall.at[2 * at + k], sibling)

    def ring_step(distance, chunk):
        for way in range(2):
            if distance < 4 or (chunk < chunks // 2) == (way == 0):
                pass_on(way, distance, chunk)

    steps = [(d, c) for d in (1, 2, 3) for c in range(chunks)] + [
        (4, c) for pair in range(chunks // 2) for c in (pair, pair + chunks // 2)
    ]

    def ring_end():
        for slot in range(8):
            at = z if slot == 0 else z_of(0 if slot < 5 else 1, slot if slot < 5 else slot - 4)
            over[slot].arrived(pall.at[2 * at + 1 - k], sibling)
        for slot in range(8):
            keep(slot).wait()

    def meet():
        code_step(3, "arrived")
        pcs, scs = pcode[...], scode[...]
        q = qc[None]
        match = ((pcs >> 3) == (q >> 3)) & ((scs >> 3) == (pcs & 7)) & ((scs & 7) == (q & 7))
        match = match & (pcs >= 0) & (scs >= 0) & (q >= 0)
        found = jnp.where(match, lax.broadcasted_iota(jnp.int32, (16, 8, B), 1) + 1, 0)
        found = jnp.sum(found, axis=1)
        source = lax.broadcasted_iota(jnp.int32, (B, B), 0)
        target = lax.broadcasted_iota(jnp.int32, (B, B), 1)

        def add_up(left, right):
            return jnp.dot(
                left.astype(jnp.bfloat16), right.astype(jnp.bfloat16), preferred_element_type=jnp.float32
            )

        def flag(condition):
            return condition.astype(jnp.float32)

        there = flag(found > 0)
        counts = add_up(there, flag((target == 64 + (source >> 3)) | (target == 72)))
        lane16 = lax.broadcasted_iota(jnp.int32, (16, B), 1)
        sidx_v[0:16, :] = jnp.where(lane16 < 64, found, counts.astype(jnp.int32))
        tile_to = lax.broadcasted_iota(jnp.int32, (16, 16), 0)
        tile_from = lax.broadcasted_iota(jnp.int32, (16, 16), 1)
        before = add_up(add_up(flag(tile_from < tile_to), there), flag(source >= 0))
        spot = before + add_up(there, flag(source <= target)) - 1.0
        spot = jnp.where((found > 0) & (spot < 128.0), spot, 255.0)
        spot = lax.dot_general(
            flag(source == target).astype(jnp.bfloat16), spot.astype(jnp.bfloat16), (((1,), (1,)), ((), ())),
            preferred_element_type=jnp.float32,
        ).astype(jnp.int32)
        tile16 = lax.broadcasted_iota(jnp.int32, (16, B), 0)
        high = (tile16 * 4 + (lane16 >> 4)).astype(jnp.float32)
        low = ((lane16 & 15) * 16 + found - 1).astype(jnp.float32)
        high_sum = jnp.zeros((1, B), jnp.float32)
        low_sum = jnp.zeros((1, B), jnp.float32)
        for t in range(16):
            hit = flag(spot[:, t : t + 1] == target)
            high_sum += add_up(high[t : t + 1], hit)
            low_sum += add_up(low[t : t + 1], hit)
        sidx_v[16:17, :] = high_sum.astype(jnp.int32) * 256 + low_sum.astype(jnp.int32)
        whole = add_up(flag(tile_from[0:8] >= 0), counts)
        sidx_v[24:32, :] = whole.astype(jnp.int32)
        pltpu.make_async_copy(sidx_v, sidx, local_sem.at[3]).start()

    def density():
        for s in range(8):
            a = p_slots[s] >> 3
            b = p_slots[s] & 7
            left = own[a]
            right = jnp.concatenate([pan[i, b] for i in range(16)], axis=1)
            raw = lax.dot_general(left, right, (((1,), (1,)), ((), ())), preferred_element_type=jnp.float32)
            raw = jnp.where(jnp.full((B, B), p_count[0], jnp.int32) > s, raw, 0.0)
            dens[s] = raw.astype(jnp.bfloat16)

    relays = [(j, side) for j in range(4) for side in range(2)]

    def inter_step(j, side):
        for half in range(2):
            inter.relay_second(half, j, side)

    def turn(core):
        def own(wave):
            for half in range(2):
                for chunk in range(2 * wave, 2 * wave + 2):
                    scattered(half, chunk)
                panel.first(2 * wave + half)
                panel.second(2 * wave + half, 0)

        def near(wave):
            for side in range(2):
                for half in range(2):
                    panel.relay_first(2 * wave + half, side)
                    panel.second(2 * wave + half, 1 + side)

        def far(wave):
            for half in range(2):
                panel.far_first(2 * wave + half)
                panel.second(2 * wave + half, 3)

        def onward(wave, j):
            for side in range(2):
                for half in range(2):
                    panel.relay_second(2 * wave + half, j, side)

        own(0)
        own(1)
        near(0)
        code_step(0, "arrived")
        code_step(1, "start")
        onward(0, 0)
        near(1)
        code_step(1, "arrived")
        code_step(2, "start")
        far(0)
        onward(0, 1)
        onward(0, 2)
        onward(1, 0)
        far(1)
        onward(1, 1)
        onward(1, 2)
        code_step(2, "arrived")
        code_step(3, "start")
        onward(0, 3)
        onward(1, 3)
        for j in range(4):
            for stream in range(4):
                panel.far_second(stream, j)
        for side in range(2):
            for half in range(2):
                inter.relay_first(half, side)
        for j in range(3):
            for half in range(2):
                inter.second(half, j)
        density()
        ring_start()
        for n, step in enumerate(steps):
            ring_step(*step)
            if n == 0:
                for half in range(2):
                    inter.far_first(half)
                    inter.second(half, 3)
            if n == 1:
                meet()
            if 2 <= n < 2 + len(relays):
                inter_step(*relays[n - 2])
        done(4)
        for j in range(4):
            for half in range(2):
                inter.far_second(half, j)
        ring_end()
        keep_s.wait()
        pltpu.make_async_copy(sidx_v, sidx, local_sem.at[3]).wait()
        panel.finish()
        inter.finish()
        all_sent(g_send, codes_sent, sibling)
        all_sent(z_send, held.at[pl.ds(0, 7)], sibling)
        all_sent(x_send, held, sibling)

    turn(2)

    for chunk in range(4):
        for piece in pieces:
            piece.moved(lambda piece=piece, chunk=chunk: piece.copy_in_plane(chunk).wait_send())

            @pl.when(piece.peer != col)
            def _(piece=piece, chunk=chunk):
                piece.far(relay.at[piece.e, chunk], chunk).wait_send()


def product_kernel(sidx, pall, sall, out, dens, todo, pbuf, sbuf, count, sem, sem_p, sem_s):
    depth = pbuf.shape[0]
    col = lax.axis_index("col")
    keep = pltpu.make_async_copy(pall.at[col], dens, sem.at[0])
    keep.start()
    total = sidx[24, 72]
    count[0] = total

    def copies(i, code):
        t, p, s = code // 1024, code // 128 % 8, code % 16
        at = i % depth
        return (
            pltpu.make_async_copy(pall.at[t, p], pbuf.at[at], sem_p.at[at]),
            pltpu.make_async_copy(sall.at[t, s], sbuf.at[at], sem_s.at[at]),
        )

    def begin(i, code):
        for copy in copies(i, code):
            copy.start()

    def tile(t, _):
        @pl.when(sidx[t, 72] > 0)
        def _():
            def slot(p, _):
                @pl.when(sidx[t, 64 + p] > 0)
                def _():
                    def pair(q, _):
                        v = sidx[t, 8 * p + q]

                        @pl.when(v > 0)
                        def _():
                            n = count[0]
                            code = t * 1024 + p * 128 + q * 16 + v - 1
                            todo[n] = code
                            count[0] = n + 1

                            @pl.when(n < depth)
                            def _():
                                begin(n, code)

                        return 0

                    lax.fori_loop(0, 8, pair, 0)

                return 0

            lax.fori_loop(0, 8, slot, 0)

        return 0

    def listed(i, _):
        code = sidx[16, i]
        todo[i] = code

        @pl.when(i < depth)
        def _():
            begin(i, code)

        return 0

    @pl.when(total <= LISTED)
    def _():
        lax.fori_loop(0, total, listed, 0)

    @pl.when(total > LISTED)
    def _():
        count[0] = 0
        lax.fori_loop(0, 16, tile, 0)

    n = count[0]
    out[...] = jnp.zeros_like(out)

    def work(first, size):
        sums = []
        for i in [first + g for g in range(size)]:
            code = todo[i]
            for copy in copies(i, code):
                copy.wait()
            at = i % depth
            sums.append((code // 16 % 8, jnp.dot(pbuf[at], sbuf[at], preferred_element_type=jnp.float32)))
        for g, (q, block) in enumerate(sums):
            out[q] += block

            @pl.when(first + g + depth < n)
            def _(g=g):
                begin(first + g + depth, todo[first + g + depth])

        return 0

    lax.fori_loop(0, n // 4, lambda i, _: work(4 * i, 4), 0)
    lax.fori_loop(n // 4 * 4, n, lambda i, _: work(i, 1), 0)
    keep.wait()


def on_device(coeffs, p_slots, p_count, s_blocks, s_slots, s_count, q_slots, q_count):
    rows, orbitals = coeffs.shape
    n = 16
    smem = pl.BlockSpec(memory_space=pltpu.SMEM)
    vmem = pl.BlockSpec(memory_space=pltpu.VMEM)
    anyspace = pl.BlockSpec(memory_space=pl.ANY)
    gathered = jax.ShapeDtypeStruct((n, rows // B, B, B), jnp.bfloat16)
    dma = pltpu.SemaphoreType.DMA
    pall, sall, sidx = pl.pallas_call(
        gather_kernel,
        out_shape=(
            gathered, gathered, jax.ShapeDtypeStruct((2 * n, B), jnp.int32),
        ),
        in_specs=[anyspace, anyspace] + [smem] * 6,
        out_specs=(anyspace, anyspace, anyspace),
        scratch_shapes=[
            pltpu.VMEM((rows // B, B, orbitals), jnp.bfloat16),
            pltpu.VMEM((n, rows // B, B, B), jnp.bfloat16),
            pltpu.VMEM((rows // B, B, B), jnp.bfloat16),
            pltpu.VMEM((rows // B, B, B), jnp.bfloat16),
            pltpu.VMEM((8, rows // B, B, B), jnp.bfloat16),
            pltpu.VMEM((2, rows // B // 2, B, B), jnp.bfloat16),
            pltpu.VMEM((2 * n, 8, B), jnp.int32),
            pltpu.VMEM((2 * n, B), jnp.int32),
            dma((4,)), dma((2, 4)), dma((2, 4)), dma((2, 4)), dma((2, 4)),
            dma((1,)), dma((80,)), dma((1,)), dma((8,)), dma((1,)), dma((40,)), dma((1,)), dma((28,)),
            dma((1,)), dma((8,)), dma((8,)),
        ],
        compiler_params=pltpu.CompilerParams(collective_id=0, has_side_effects=True),
        name="gather",
    )(
        coeffs.reshape(rows // B, B, orbitals), s_blocks.reshape(rows // B, B, B), p_slots.reshape(8), p_count.reshape(1), s_slots.reshape(8),
        s_count.reshape(1), q_slots.reshape(8), q_count.reshape(1),
    )
    depth = 32
    product, dens = pl.pallas_call(
        product_kernel,
        out_shape=(
            jax.ShapeDtypeStruct((8, B, B), jnp.float32), jax.ShapeDtypeStruct((8, B, B), jnp.bfloat16)
        ),
        in_specs=[smem, anyspace, anyspace],
        out_specs=(vmem, vmem),
        scratch_shapes=[
            pltpu.SMEM((1024,), jnp.int32),
            pltpu.VMEM((depth, B, B), jnp.bfloat16),
            pltpu.VMEM((depth, B, B), jnp.bfloat16),
            pltpu.SMEM((1,), jnp.int32),
            dma((1,)), dma((depth,)), dma((depth,)),
        ],
        name="product",
    )(sidx, pall, sall)
    return dens.reshape(1, 1, 8, B, B), product.reshape(1, 1, 8, B, B)


def solution(mesh):
    return jax.shard_map(
        on_device,
        mesh=mesh,
        in_specs=(
            P("row", None),
            P("row", "col", None),
            P("row", "col"),
            P("row", "col", None, None, None),
            P("row", "col", None),
            P("row", "col"),
            P("row", "col", None),
            P("row", "col"),
        ),
        out_specs=(P("row", "col", None, None, None), P("row", "col", None, None, None)),
        check_vma=False,
    )
```

```python
import functools

import jax
import jax.numpy as jnp
from jax import lax
from jax.experimental import pallas as pl
from jax.experimental.pallas import tpu as pltpu
from jax.sharding import PartitionSpec as P

MESH = pl.DeviceIdType.MESH
B = 128
LISTED = 128
FIRST = (8, 11, 6, 9, 14, 7, 10, 5)
SECOND = (2, 1, 12, 3, 4, 13, 0, 15)
PLANE = tuple((FIRST if i in FIRST else SECOND).index(i) for i in range(16))


def lookup(table, at):
    value = 0
    for base in range(0, len(table), 4):
        packed = sum(table[base + i] << (4 * i) for i in range(4))
        inside = (at // 4 == base // 4).astype(jnp.int32)
        value = value + inside * ((packed // (1 << (4 * (at % 4)))) % 16)
    return value


class Link:
    def __init__(self, send, recv, at):
        self.send, self.recv, self.at = send, recv, at

    def start(self, src, dst, device):
        pltpu.make_async_remote_copy(
            src_ref=src, dst_ref=dst, send_sem=self.send.at[0], recv_sem=self.recv.at[self.at],
            device_id=device, device_id_type=MESH,
        ).start()

    def arrived(self, landing, device):
        pltpu.make_async_remote_copy(
            src_ref=landing, dst_ref=landing, send_sem=self.send.at[0], recv_sem=self.recv.at[self.at],
            device_id=device, device_id_type=MESH,
        ).wait_recv()


def all_sent(send, whole, device):
    pltpu.make_async_remote_copy(
        src_ref=whole, dst_ref=whole, send_sem=send.at[0], recv_sem=send.at[0], device_id=device, device_id_type=MESH
    ).wait_send()


class PlaneGather:
    def __init__(self, buf, own, send, recv, place, streams):
        self.buf, self.own = buf, own
        self.y, self.x, self.col = place
        self.size = own.shape[0] // streams
        self.links = [Link(send, recv, m) for m in range(12 * streams + 1)]

    def index(self, stream, du, dv):
        if stream % 2 == 0:
            return 4 * ((self.y + dv + 4) % 4) + (self.x + du + 4) % 4
        return 4 * ((self.y + du + 4) % 4) + (self.x + dv + 4) % 4

    def device(self, stream, du, dv):
        return (self.index(stream, du, dv), self.col)

    def span(self, stream, part):
        base = (stream % 2) * self.own.shape[0] // 2 + (stream // 2) * self.size
        if part is None:
            return pl.ds(base, self.size)
        return pl.ds(base + part * (self.size // 2), self.size // 2)

    def block(self, stream, du, dv, part=None):
        return self.buf.at[self.index(stream, du, dv), self.span(stream, part)]

    def link(self, stream, number):
        return self.links[12 * stream + number]

    def first(self, stream):
        src = self.own.at[self.span(stream, None)]
        dst = self.block(stream, 0, 0)
        self.link(stream, 0).start(src, dst, self.device(stream, 1, 0))
        self.link(stream, 1).start(src, dst, self.device(stream, -1, 0))

    def relay_first(self, stream, side):
        du = -1 if side == 0 else 1
        self.link(stream, side).arrived(self.block(stream, du, 0), self.device(stream, du, 0))
        part = self.block(stream, du, 0, side)
        self.link(stream, 2 + side).start(part, part, self.device(stream, -du, 0))

    def far_first(self, stream):
        for side in range(2):
            part = self.block(stream, 2, 0, side)
            self.link(stream, 2 + side).arrived(part, self.device(stream, -1 if side == 0 else 1, 0))

    def second(self, stream, j):
        du = (0, -1, 1, 2)[j]
        dst = self.block(stream, du, 0)
        src = self.own.at[self.span(stream, None)] if j == 0 else dst
        self.link(stream, 4 + 2 * j).start(src, dst, self.device(stream, 0, 1))
        self.link(stream, 5 + 2 * j).start(src, dst, self.device(stream, 0, -1))

    def relay_second(self, stream, j, side):
        du = (0, -1, 1, 2)[j]
        dv = -1 if side == 0 else 1
        number = 4 + 2 * j + side
        self.link(stream, number).arrived(self.block(stream, du, dv), self.device(stream, 0, dv))
        part = self.block(stream, du, dv, side)
        self.links[-1].start(part, part, self.device(stream, 0, -dv))

    def far_second(self):
        self.links[-1].arrived(self.buf.at[pl.ds(0, 4)], self.device(0, 0, 1))

    def finish(self):
        all_sent(self.links[0].send, self.buf.at[pl.ds(0, 15)], self.device(0, 1, 0))


def gather_kernel(
    coeffs, sblk, p_slots, p_count, s_slots, s_count, q_slots, q_count,
    pall, sall, sidx,
    own, pan, sown, dens, held, relay, code_v, sidx_v,
    local_sem, plane_send, plane_recv, far_send, far_recv, c_send, c_recv, g_send, g_recv, s_send, s_recv, z_send, z_recv,
    x_send, x_recv, keep_sem,
):
    row = lax.axis_index("row")
    col = lax.axis_index("col")
    pcode, scode = code_v.at[pl.ds(0, 16)], code_v.at[pl.ds(16, 16)]
    codes_sent = code_v.at[pl.ds(0, 30)]
    y, x = row // 4, row % 4
    z, k = col // 2, col % 2

    load_own = pltpu.make_async_copy(coeffs, own, local_sem.at[0])
    load_s = pltpu.make_async_copy(sblk, sown, local_sem.at[1])
    load_own.start()
    load_s.start()

    barrier = pltpu.get_barrier_semaphore()
    for j in range(1, 16):
        pl.semaphore_signal(barrier, inc=1, device_id=(row, (col + j) % 16), device_id_type=MESH)
        pl.semaphore_signal(barrier, inc=1, device_id=((row + j) % 16, col), device_id_type=MESH)

    lane = lax.broadcasted_iota(jnp.int32, (8, B), 1)
    sub = lax.broadcasted_iota(jnp.int32, (8, B), 0)
    pc = jnp.full((8, B), -1, jnp.int32)
    qc = jnp.full((8, B), -100, jnp.int32)
    sc = jnp.full((8, B), -1, jnp.int32)
    p_live = jnp.full((8, B), p_count[0], jnp.int32)
    q_live = jnp.full((8, B), q_count[0], jnp.int32)
    s_live = jnp.full((8, B), s_count[0], jnp.int32)
    for i in range(8):
        pc = jnp.where((lane // 8 == i) & (p_live > i), jnp.full((8, B), p_slots[i], jnp.int32), pc)
        qc = jnp.where(
            (lane % 8 == i) & (lane < 64) & (q_live > i), jnp.full((8, B), q_slots[i], jnp.int32), qc
        )
        sc = jnp.where((sub == i) & (s_live > i), jnp.full((8, B), s_slots[i], jnp.int32), sc)
    pcode[col] = pc
    scode[row] = sc

    load_own.wait()
    load_s.wait()

    pl.semaphore_wait(barrier, 30)

    def slice_of(at, chunk):
        return own.at[4 * k + chunk, :, pl.ds(pl.multiple_of(at * B, B), B)]

    class Piece:
        def __init__(self, e, table):
            self.shift = lookup(table, z)
            self.e, self.moves = e, 0 not in table
            self.peer = row ^ self.shift

        def copy_in_plane(self, chunk):
            return pltpu.make_async_remote_copy(
                src_ref=slice_of(self.peer, chunk), dst_ref=relay.at[self.e, chunk],
                send_sem=plane_send.at[self.e], recv_sem=plane_recv.at[self.e, chunk],
                device_id=(self.peer, col), device_id_type=MESH,
            )

        def moved(self, act):
            if self.moves:
                act()
            else:
                pl.when(self.shift != 0)(act)

        def stays(self, act):
            if not self.moves:
                pl.when(self.shift == 0)(act)

        def far(self, src, chunk):
            return pltpu.make_async_remote_copy(
                src_ref=src, dst_ref=pan.at[row, 4 * k + chunk],
                send_sem=far_send.at[self.e], recv_sem=far_recv.at[k, chunk],
                device_id=(row, self.peer), device_id_type=MESH,
            )

        def hand_on(self, src, chunk):
            @pl.when(self.peer == col)
            def _():
                pltpu.make_async_copy(src, pan.at[row, 4 * k + chunk], far_recv.at[k, chunk]).start()

            @pl.when(self.peer != col)
            def _():
                self.far(src, chunk).start()

    pieces = [Piece(0, FIRST), Piece(1, SECOND)]
    for chunk in range(4):
        for piece in pieces:
            piece.moved(lambda piece=piece, chunk=chunk: piece.copy_in_plane(chunk).start())
            piece.stays(lambda piece=piece, chunk=chunk: piece.hand_on(slice_of(row, chunk), chunk))

    place = (y, x, col)
    panel = PlaneGather(pan, pan.at[row], c_send, c_recv, place, 4)
    inter = PlaneGather(sall, sown, s_send, s_recv, place, 2)
    keep_s = pltpu.make_async_copy(sown, sall.at[row], local_sem.at[2])
    keep_s.start()

    for chunk in range(4):
        for piece in pieces:

            def pass_along(piece=piece, chunk=chunk):
                piece.copy_in_plane(chunk).wait_recv()
                piece.hand_on(relay.at[piece.e, chunk], chunk)

            piece.moved(pass_along)

    for half in range(2):
        inter.first(half)
    codes = [Link(g_send, g_recv, m) for m in range(8)]

    def code_step(step, act):
        size = 1 << step
        for dim, (ref, me) in enumerate(((pcode, col), (scode, row))):
            mine = me // size * size
            other = me ^ size
            device = (row, other) if dim == 0 else (other, col)
            if act == "start":
                here = ref.at[pl.ds(mine, size)]
                codes[2 * step + dim].start(here, here, device)
            else:
                codes[2 * step + dim].arrived(ref.at[pl.ds(mine ^ size, size)], device)

    code_step(0, "start")

    my_plane = lookup(PLANE, row ^ col)

    def scattered(half, chunk):
        by_me = (my_plane == z) & (k == half)
        landing = pan.at[row, 4 * half + chunk]

        @pl.when(by_me)
        def _():
            pltpu.make_async_copy(landing, landing, far_recv.at[half, chunk]).wait()

        @pl.when(jnp.logical_not(by_me))
        def _():
            pltpu.make_async_remote_copy(
                src_ref=landing, dst_ref=landing, send_sem=far_send.at[0],
                recv_sem=far_recv.at[half, chunk],
                device_id=(row, col + 1 - 2 * k), device_id_type=MESH,
            ).wait_recv()

    sibling = (row, col + 1 - 2 * k)
    up = (row, (col + 2) % 16)
    down = (row, (col + 14) % 16)
    chunks = 4
    size = dens.shape[0] // chunks
    ring = [Link(z_send, z_recv, m) for m in range(7 * chunks)]
    over = Link(x_send, x_recv, 0)

    def number(way, distance, chunk):
        return 7 * chunks // 2 * way + (
            chunks * (distance - 1) + chunk if distance < 4 else 3 * chunks + chunk % (chunks // 2)
        )

    def z_of(way, distance):
        return (z + 8 - distance) % 8 if way == 0 else (z + distance) % 8

    def part(ref, chunk):
        return ref.at[pl.ds(chunk * size, size)]

    def ring_start(chunk):
        for way in range(2):
            ring[number(way, 1, chunk)].start(
                part(dens, chunk), part(held.at[z], chunk), up if way == 0 else down
            )

    def share(at, first, count):
        src = (dens if at is None else held.at[at]).at[pl.ds(first, count)]
        dst = pall.at[col if at is None else 2 * at + k, pl.ds(first, count)]
        pltpu.make_async_copy(src, dst, keep_sem.at[0]).start()
        over.start(src, dst, sibling)

    def goes_on(way, distance, chunk):
        return distance < 3 or (distance == 3 and (chunk < chunks // 2) == (way == 0))

    def pass_on(way, distance, chunk):
        here = part(held.at[z_of(way, distance)], chunk)
        ring[number(way, distance, chunk)].arrived(here, down if way == 0 else up)
        if goes_on(way, distance, chunk):
            ring[number(way, distance + 1, chunk)].start(here, here, up if way == 0 else down)
        if distance < 4 and chunk == chunks - 1:
            share(z_of(way, distance), 0, dens.shape[0])
        if distance == 4 and chunk % (chunks // 2) == chunks // 2 - 1:
            share(z_of(way, 4), way * (dens.shape[0] // 2), dens.shape[0] // 2)

    def ring_step(distance, chunk):
        for way in range(2):
            if distance < 4 or (chunk < chunks // 2) == (way == 0):
                pass_on(way, distance, chunk)

    steps = [(d, c) for d in (1, 2, 3) for c in range(chunks)] + [
        (4, c) for pair in range(chunks // 2) for c in (pair, pair + chunks // 2)
    ]

    def ring_end():
        over.arrived(pall.at[pl.ds(0, 8)], sibling)
        pltpu.make_async_copy(held, pall.at[pl.ds(0, 8)], keep_sem.at[0]).wait()

    def meet():
        code_step(3, "arrived")
        pcs, scs = pcode[...], scode[...]
        q = qc[None]
        match = ((pcs >> 3) == (q >> 3)) & ((scs >> 3) == (pcs & 7)) & ((scs & 7) == (q & 7))
        match = match & (pcs >= 0) & (scs >= 0) & (q >= 0)
        found = jnp.where(match, lax.broadcasted_iota(jnp.int32, (16, 8, B), 1) + 1, 0)
        found = jnp.sum(found, axis=1)
        source = lax.broadcasted_iota(jnp.int32, (B, B), 0)
        target = lax.broadcasted_iota(jnp.int32, (B, B), 1)

        def add_up(left, right):
            return jnp.dot(
                left.astype(jnp.bfloat16), right.astype(jnp.bfloat16), preferred_element_type=jnp.float32
            )

        def flag(condition):
            return condition.astype(jnp.float32)

        there = flag(found > 0)
        counts = add_up(there, flag((target == 64 + (source >> 3)) | (target == 72)))
        lane16 = lax.broadcasted_iota(jnp.int32, (16, B), 1)
        sidx_v[0:16, :] = jnp.where(lane16 < 64, found, counts.astype(jnp.int32))
        tile_to = lax.broadcasted_iota(jnp.int32, (16, 16), 0)
        tile_from = lax.broadcasted_iota(jnp.int32, (16, 16), 1)
        before = add_up(add_up(flag(tile_from < tile_to), there), flag(source >= 0))
        spot = before + add_up(there, flag(source <= target)) - 1.0
        spot = jnp.where((found > 0) & (spot < 128.0), spot, 255.0)
        spot = lax.dot_general(
            flag(source == target).astype(jnp.bfloat16), spot.astype(jnp.bfloat16), (((1,), (1,)), ((), ())),
            preferred_element_type=jnp.float32,
        ).astype(jnp.int32)
        tile16 = lax.broadcasted_iota(jnp.int32, (16, B), 0)
        high = (tile16 * 4 + (lane16 >> 4)).astype(jnp.float32)
        low = ((lane16 & 15) * 16 + found - 1).astype(jnp.float32)
        high_sum = jnp.zeros((1, B), jnp.float32)
        low_sum = jnp.zeros((1, B), jnp.float32)
        for t in range(16):
            hit = flag(spot[:, t : t + 1] == target)
            high_sum += add_up(high[t : t + 1], hit)
            low_sum += add_up(low[t : t + 1], hit)
        sidx_v[16:17, :] = high_sum.astype(jnp.int32) * 256 + low_sum.astype(jnp.int32)
        whole = add_up(flag(tile_from[0:8] >= 0), counts)
        sidx_v[24:32, :] = whole.astype(jnp.int32)
        pltpu.make_async_copy(sidx_v, sidx, local_sem.at[3]).start()

    def density():
        for s in range(8):
            a = p_slots[s] >> 3
            b = p_slots[s] & 7
            left = own[a]
            right = jnp.concatenate([pan[i, b] for i in range(16)], axis=1)
            raw = lax.dot_general(left, right, (((1,), (1,)), ((), ())), preferred_element_type=jnp.float32)
            raw = jnp.where(jnp.full((B, B), p_count[0], jnp.int32) > s, raw, 0.0)
            dens[s] = raw.astype(jnp.bfloat16)
            if s % size == size - 1 and s >= size:
                ring_start(s // size - 1)
        ring_start(chunks - 1)
        share(None, 0, dens.shape[0])

    relays = [(j, side) for j in range(4) for side in range(2)]

    def inter_step(j, side):
        for half in range(2):
            inter.relay_second(half, j, side)

    def turn(core):
        def own(wave):
            for half in range(2):
                for chunk in range(2 * wave, 2 * wave + 2):
                    scattered(half, chunk)
                panel.first(2 * wave + half)
                panel.second(2 * wave + half, 0)

        def near(wave):
            for side in range(2):
                for half in range(2):
                    panel.relay_first(2 * wave + half, side)
                    panel.second(2 * wave + half, 1 + side)

        def far(wave):
            for half in range(2):
                panel.far_first(2 * wave + half)
                panel.second(2 * wave + half, 3)

        def onward(wave, j):
            for side in range(2):
                for half in range(2):
                    panel.relay_second(2 * wave + half, j, side)

        own(0)
        own(1)
        near(0)
        code_step(0, "arrived")
        code_step(1, "start")
        onward(0, 0)
        near(1)
        code_step(1, "arrived")
        code_step(2, "start")
        far(0)
        onward(0, 1)
        onward(0, 2)
        onward(1, 0)
        far(1)
        onward(1, 1)
        onward(1, 2)
        code_step(2, "arrived")
        code_step(3, "start")
        onward(0, 3)
        onward(1, 3)
        panel.far_second()
        for side in range(2):
            for half in range(2):
                inter.relay_first(half, side)
        for j in range(3):
            for half in range(2):
                inter.second(half, j)
        density()
        for n, step in enumerate(steps):
            ring_step(*step)
            if n == 0:
                for half in range(2):
                    inter.far_first(half)
                    inter.second(half, 3)
            if n == 1:
                meet()
            if 2 <= n < 2 + len(relays):
                inter_step(*relays[n - 2])
        inter.far_second()
        ring_end()
        keep_s.wait()
        pltpu.make_async_copy(sidx_v, sidx, local_sem.at[3]).wait()
        panel.finish()
        inter.finish()
        all_sent(g_send, codes_sent, sibling)
        all_sent(z_send, held.at[pl.ds(0, 7)], sibling)
        all_sent(x_send, held, sibling)

    turn(2)

    for piece in pieces:

        def left(sems, piece=piece):
            whole = relay.at[piece.e]
            pltpu.make_async_remote_copy(
                src_ref=whole, dst_ref=whole, send_sem=sems.at[piece.e], recv_sem=sems.at[piece.e],
                device_id=sibling, device_id_type=MESH,
            ).wait_send()

        piece.moved(functools.partial(left, plane_send))
        pl.when(piece.peer != col)(functools.partial(left, far_send))


def product_kernel(sidx, pall, sall, out, dens, todo, pbuf, sbuf, count, sem, sem_p, sem_s):
    depth = pbuf.shape[0]
    col = lax.axis_index("col")
    keep = pltpu.make_async_copy(pall.at[col], dens, sem.at[0])
    keep.start()
    total = sidx[24, 72]
    count[0] = total

    def copies(i, code):
        t, p, s = code // 1024, code // 128 % 8, code % 16
        at = i % depth
        return (
            pltpu.make_async_copy(pall.at[t, p], pbuf.at[at], sem_p.at[at]),
            pltpu.make_async_copy(sall.at[t, s], sbuf.at[at], sem_s.at[at]),
        )

    def begin(i, code):
        for copy in copies(i, code):
            copy.start()

    def tile(t, _):
        @pl.when(sidx[t, 72] > 0)
        def _():
            def slot(p, _):
                @pl.when(sidx[t, 64 + p] > 0)
                def _():
                    def pair(q, _):
                        v = sidx[t, 8 * p + q]

                        @pl.when(v > 0)
                        def _():
                            n = count[0]
                            code = t * 1024 + p * 128 + q * 16 + v - 1
                            todo[n] = code
                            count[0] = n + 1

                            @pl.when(n < depth)
                            def _():
                                begin(n, code)

                        return 0

                    lax.fori_loop(0, 8, pair, 0)

                return 0

            lax.fori_loop(0, 8, slot, 0)

        return 0

    def listed(i, _):
        code = sidx[16, i]
        todo[i] = code

        @pl.when(i < depth)
        def _():
            begin(i, code)

        return 0

    @pl.when(total <= LISTED)
    def _():
        lax.fori_loop(0, total, listed, 0)

    @pl.when(total > LISTED)
    def _():
        count[0] = 0
        lax.fori_loop(0, 16, tile, 0)

    n = count[0]
    out[...] = jnp.zeros_like(out)

    def work(first, size):
        sums = []
        for i in [first + g for g in range(size)]:
            code = todo[i]
            for copy in copies(i, code):
                copy.wait()
            at = i % depth
            sums.append((code // 16 % 8, jnp.dot(pbuf[at], sbuf[at], preferred_element_type=jnp.float32)))
        for g, (q, block) in enumerate(sums):
            out[q] += block

            @pl.when(first + g + depth < n)
            def _(g=g):
                begin(first + g + depth, todo[first + g + depth])

        return 0

    lax.fori_loop(0, n // 4, lambda i, _: work(4 * i, 4), 0)
    lax.fori_loop(n // 4 * 4, n, lambda i, _: work(i, 1), 0)
    keep.wait()


def on_device(coeffs, p_slots, p_count, s_blocks, s_slots, s_count, q_slots, q_count):
    rows, orbitals = coeffs.shape
    n = 16
    smem = pl.BlockSpec(memory_space=pltpu.SMEM)
    vmem = pl.BlockSpec(memory_space=pltpu.VMEM)
    anyspace = pl.BlockSpec(memory_space=pl.ANY)
    gathered = jax.ShapeDtypeStruct((n, rows // B, B, B), jnp.bfloat16)
    dma = pltpu.SemaphoreType.DMA
    pall, sall, sidx = pl.pallas_call(
        gather_kernel,
        out_shape=(
            gathered, gathered, jax.ShapeDtypeStruct((2 * n, B), jnp.int32),
        ),
        in_specs=[anyspace, anyspace] + [smem] * 6,
        out_specs=(anyspace, anyspace, anyspace),
        scratch_shapes=[
            pltpu.VMEM((rows // B, B, orbitals), jnp.bfloat16),
            pltpu.VMEM((n, rows // B, B, B), jnp.bfloat16),
            pltpu.VMEM((rows // B, B, B), jnp.bfloat16),
            pltpu.VMEM((rows // B, B, B), jnp.bfloat16),
            pltpu.VMEM((8, rows // B, B, B), jnp.bfloat16),
            pltpu.VMEM((2, rows // B // 2, B, B), jnp.bfloat16),
            pltpu.VMEM((2 * n, 8, B), jnp.int32),
            pltpu.VMEM((2 * n, B), jnp.int32),
            dma((4,)), dma((2,)), dma((2, 4)), dma((2,)), dma((2, 4)),
            dma((1,)), dma((49,)), dma((1,)), dma((8,)), dma((1,)), dma((25,)), dma((1,)), dma((28,)),
            dma((1,)), dma((1,)), dma((1,)),
        ],
        compiler_params=pltpu.CompilerParams(collective_id=0, has_side_effects=True),
        name="gather",
    )(
        coeffs.reshape(rows // B, B, orbitals), s_blocks.reshape(rows // B, B, B), p_slots.reshape(8), p_count.reshape(1), s_slots.reshape(8),
        s_count.reshape(1), q_slots.reshape(8), q_count.reshape(1),
    )
    depth = 32
    product, dens = pl.pallas_call(
        product_kernel,
        out_shape=(
            jax.ShapeDtypeStruct((8, B, B), jnp.float32), jax.ShapeDtypeStruct((8, B, B), jnp.bfloat16)
        ),
        in_specs=[smem, anyspace, anyspace],
        out_specs=(vmem, vmem),
        scratch_shapes=[
            pltpu.SMEM((1024,), jnp.int32),
            pltpu.VMEM((depth, B, B), jnp.bfloat16),
            pltpu.VMEM((depth, B, B), jnp.bfloat16),
            pltpu.SMEM((1,), jnp.int32),
            dma((1,)), dma((depth,)), dma((depth,)),
        ],
        name="product",
    )(sidx, pall, sall)
    return dens.reshape(1, 1, 8, B, B), product.reshape(1, 1, 8, B, B)


def solution(mesh):
    return jax.shard_map(
        on_device,
        mesh=mesh,
        in_specs=(
            P("row", None),
            P("row", "col", None),
            P("row", "col"),
            P("row", "col", None, None, None),
            P("row", "col", None),
            P("row", "col"),
            P("row", "col", None),
            P("row", "col"),
        ),
        out_specs=(P("row", "col", None, None, None), P("row", "col", None, None, None)),
        check_vma=False,
    )
```

```python
import functools

import jax
import jax.numpy as jnp
from jax import lax
from jax.experimental import pallas as pl
from jax.experimental.pallas import tpu as pltpu
from jax.sharding import PartitionSpec as P

MESH = pl.DeviceIdType.MESH
B = 128
LISTED = 128
FIRST = (8, 11, 6, 9, 14, 7, 10, 5)
SECOND = (2, 1, 12, 3, 4, 13, 0, 15)
PLANE = tuple((FIRST if i in FIRST else SECOND).index(i) for i in range(16))


def lookup(table, at):
    value = 0
    for base in range(0, len(table), 4):
        packed = sum(table[base + i] << (4 * i) for i in range(4))
        inside = (at // 4 == base // 4).astype(jnp.int32)
        value = value + inside * ((packed // (1 << (4 * (at % 4)))) % 16)
    return value


class Link:
    def __init__(self, send, recv, at):
        self.send, self.recv, self.at = send, recv, at

    def start(self, src, dst, device):
        pltpu.make_async_remote_copy(
            src_ref=src, dst_ref=dst, send_sem=self.send.at[0], recv_sem=self.recv.at[self.at],
            device_id=device, device_id_type=MESH,
        ).start()

    def arrived(self, landing, device):
        pltpu.make_async_remote_copy(
            src_ref=landing, dst_ref=landing, send_sem=self.send.at[0], recv_sem=self.recv.at[self.at],
            device_id=device, device_id_type=MESH,
        ).wait_recv()


def all_sent(send, whole, device):
    pltpu.make_async_remote_copy(
        src_ref=whole, dst_ref=whole, send_sem=send.at[0], recv_sem=send.at[0], device_id=device, device_id_type=MESH
    ).wait_send()


class PlaneGather:
    def __init__(self, buf, own, send, recv, place, streams):
        self.buf, self.own = buf, own
        self.y, self.x, self.col = place
        self.size = own.shape[0] // streams
        self.links = [Link(send, recv, m) for m in range(12 * streams + 1)]

    def index(self, stream, du, dv):
        if stream % 2 == 0:
            return 4 * ((self.y + dv + 4) % 4) + (self.x + du + 4) % 4
        return 4 * ((self.y + du + 4) % 4) + (self.x + dv + 4) % 4

    def device(self, stream, du, dv):
        return (self.index(stream, du, dv), self.col)

    def span(self, stream, part):
        base = (stream % 2) * self.own.shape[0] // 2 + (stream // 2) * self.size
        if part is None:
            return pl.ds(base, self.size)
        return pl.ds(base + part * (self.size // 2), self.size // 2)

    def block(self, stream, du, dv, part=None):
        return self.buf.at[self.index(stream, du, dv), self.span(stream, part)]

    def link(self, stream, number):
        return self.links[12 * stream + number]

    def first(self, stream):
        src = self.own.at[self.span(stream, None)]
        dst = self.block(stream, 0, 0)
        self.link(stream, 0).start(src, dst, self.device(stream, 1, 0))
        self.link(stream, 1).start(src, dst, self.device(stream, -1, 0))

    def relay_first(self, stream, side):
        du = -1 if side == 0 else 1
        self.link(stream, side).arrived(self.block(stream, du, 0), self.device(stream, du, 0))
        part = self.block(stream, du, 0, side)
        self.link(stream, 2 + side).start(part, part, self.device(stream, -du, 0))

    def far_first(self, stream):
        for side in range(2):
            part = self.block(stream, 2, 0, side)
            self.link(stream, 2 + side).arrived(part, self.device(stream, -1 if side == 0 else 1, 0))

    def second(self, stream, j):
        du = (0, -1, 1, 2)[j]
        dst = self.block(stream, du, 0)
        src = self.own.at[self.span(stream, None)] if j == 0 else dst
        self.link(stream, 4 + 2 * j).start(src, dst, self.device(stream, 0, 1))
        self.link(stream, 5 + 2 * j).start(src, dst, self.device(stream, 0, -1))

    def relay_second(self, stream, j, side):
        du = (0, -1, 1, 2)[j]
        dv = -1 if side == 0 else 1
        number = 4 + 2 * j + side
        self.link(stream, number).arrived(self.block(stream, du, dv), self.device(stream, 0, dv))
        part = self.block(stream, du, dv, side)
        self.links[-1].start(part, part, self.device(stream, 0, -dv))

    def far_second(self):
        self.links[-1].arrived(self.buf.at[pl.ds(0, 4)], self.device(0, 0, 1))

    def finish(self):
        all_sent(self.links[0].send, self.buf.at[pl.ds(0, 15)], self.device(0, 1, 0))


def gather_kernel(
    coeffs, sblk, p_slots_in, p_count_in, s_slots_in, s_count_in, q_slots_in, q_count_in,
    pall, sall, pairs, table,
    p_slots, p_count, s_slots, s_count, q_slots, q_count,
    own, pan, sown, dens, held, relay, code_v, pairs_v, table_v,
    local_sem, plane_send, plane_recv, far_send, far_recv, c_send, c_recv, g_send, g_recv, s_send, s_recv, z_send, z_recv,
    x_send, x_recv, keep_sem, small_sem,
):
    row = lax.axis_index("row")
    col = lax.axis_index("col")
    pcode, scode = code_v.at[pl.ds(0, 16)], code_v.at[pl.ds(16, 16)]
    codes_sent = code_v.at[pl.ds(0, 30)]
    y, x = row // 4, row % 4
    z, k = col // 2, col % 2

    load_own = pltpu.make_async_copy(coeffs, own, local_sem.at[0])
    load_s = pltpu.make_async_copy(sblk, sown, local_sem.at[1])

    barrier = pltpu.get_barrier_semaphore()
    for j in range(1, 16):
        pl.semaphore_signal(barrier, inc=1, device_id=(row, (col + j) % 16), device_id_type=MESH)
        pl.semaphore_signal(barrier, inc=1, device_id=((row + j) % 16, col), device_id_type=MESH)

    load_own.start()
    load_s.start()
    small = [
        pltpu.make_async_copy(src, dst, small_sem.at[at])
        for at, (src, dst) in enumerate((
            (p_slots_in, p_slots), (p_count_in, p_count), (s_slots_in, s_slots),
            (s_count_in, s_count), (q_slots_in, q_slots), (q_count_in, q_count),
        ))
    ]
    for copy in small:
        copy.start()
    for copy in small:
        copy.wait()

    lane = lax.broadcasted_iota(jnp.int32, (8, B), 1)
    sub = lax.broadcasted_iota(jnp.int32, (8, B), 0)
    pc = jnp.full((8, B), -1, jnp.int32)
    qc = jnp.full((8, B), -100, jnp.int32)
    sc = jnp.full((8, B), -1, jnp.int32)
    p_live = jnp.full((8, B), p_count[0], jnp.int32)
    q_live = jnp.full((8, B), q_count[0], jnp.int32)
    s_live = jnp.full((8, B), s_count[0], jnp.int32)
    for i in range(8):
        pc = jnp.where((lane // 8 == i) & (p_live > i), jnp.full((8, B), p_slots[i], jnp.int32), pc)
        qc = jnp.where(
            (lane % 8 == i) & (lane < 64) & (q_live > i), jnp.full((8, B), q_slots[i], jnp.int32), qc
        )
        sc = jnp.where((sub == i) & (s_live > i), jnp.full((8, B), s_slots[i], jnp.int32), sc)
    pcode[col] = pc
    scode[row] = sc

    load_own.wait()
    load_s.wait()

    pl.semaphore_wait(barrier, 30)

    def slice_of(at, chunk):
        return own.at[4 * k + chunk, :, pl.ds(pl.multiple_of(at * B, B), B)]

    class Piece:
        def __init__(self, e, table):
            self.shift = lookup(table, z)
            self.e, self.moves = e, 0 not in table
            self.peer = row ^ self.shift

        def copy_in_plane(self, chunk):
            return pltpu.make_async_remote_copy(
                src_ref=slice_of(self.peer, chunk), dst_ref=relay.at[self.e, chunk],
                send_sem=plane_send.at[self.e], recv_sem=plane_recv.at[self.e, chunk],
                device_id=(self.peer, col), device_id_type=MESH,
            )

        def moved(self, act):
            if self.moves:
                act()
            else:
                pl.when(self.shift != 0)(act)

        def stays(self, act):
            if not self.moves:
                pl.when(self.shift == 0)(act)

        def far(self, src, chunk):
            return pltpu.make_async_remote_copy(
                src_ref=src, dst_ref=pan.at[row, 4 * k + chunk],
                send_sem=far_send.at[self.e], recv_sem=far_recv.at[k, chunk],
                device_id=(row, self.peer), device_id_type=MESH,
            )

        def hand_on(self, src, chunk):
            @pl.when(self.peer == col)
            def _():
                pltpu.make_async_copy(src, pan.at[row, 4 * k + chunk], far_recv.at[k, chunk]).start()

            @pl.when(self.peer != col)
            def _():
                self.far(src, chunk).start()

    pieces = [Piece(0, FIRST), Piece(1, SECOND)]
    for chunk in range(4):
        for piece in pieces:
            piece.moved(lambda piece=piece, chunk=chunk: piece.copy_in_plane(chunk).start())
            piece.stays(lambda piece=piece, chunk=chunk: piece.hand_on(slice_of(row, chunk), chunk))

    place = (y, x, col)
    panel = PlaneGather(pan, pan.at[row], c_send, c_recv, place, 4)
    inter = PlaneGather(sall, sown, s_send, s_recv, place, 2)
    keep_s = pltpu.make_async_copy(sown, sall.at[row], local_sem.at[2])
    keep_s.start()

    for chunk in range(4):
        for piece in pieces:

            def pass_along(piece=piece, chunk=chunk):
                piece.copy_in_plane(chunk).wait_recv()
                piece.hand_on(relay.at[piece.e, chunk], chunk)

            piece.moved(pass_along)

    for half in range(2):
        inter.first(half)
    codes = [Link(g_send, g_recv, m) for m in range(8)]

    def code_step(step, act):
        size = 1 << step
        for dim, (ref, me) in enumerate(((pcode, col), (scode, row))):
            mine = me // size * size
            other = me ^ size
            device = (row, other) if dim == 0 else (other, col)
            if act == "start":
                here = ref.at[pl.ds(mine, size)]
                codes[2 * step + dim].start(here, here, device)
            else:
                codes[2 * step + dim].arrived(ref.at[pl.ds(mine ^ size, size)], device)

    code_step(0, "start")

    my_plane = lookup(PLANE, row ^ col)

    def scattered(half, chunk):
        by_me = (my_plane == z) & (k == half)
        landing = pan.at[row, 4 * half + chunk]

        @pl.when(by_me)
        def _():
            pltpu.make_async_copy(landing, landing, far_recv.at[half, chunk]).wait()

        @pl.when(jnp.logical_not(by_me))
        def _():
            pltpu.make_async_remote_copy(
                src_ref=landing, dst_ref=landing, send_sem=far_send.at[0],
                recv_sem=far_recv.at[half, chunk],
                device_id=(row, col + 1 - 2 * k), device_id_type=MESH,
            ).wait_recv()

    sibling = (row, col + 1 - 2 * k)
    up = (row, (col + 2) % 16)
    down = (row, (col + 14) % 16)
    chunks = 4
    size = dens.shape[0] // chunks
    ring = [Link(z_send, z_recv, m) for m in range(7 * chunks)]
    over = Link(x_send, x_recv, 0)

    def number(way, distance, chunk):
        return 7 * chunks // 2 * way + (
            chunks * (distance - 1) + chunk if distance < 4 else 3 * chunks + chunk % (chunks // 2)
        )

    def z_of(way, distance):
        return (z + 8 - distance) % 8 if way == 0 else (z + distance) % 8

    def part(ref, chunk):
        return ref.at[pl.ds(chunk * size, size)]

    def ring_start(chunk):
        for way in range(2):
            ring[number(way, 1, chunk)].start(
                part(dens, chunk), part(held.at[z], chunk), up if way == 0 else down
            )

    def share(at, first, count):
        src = (dens if at is None else held.at[at]).at[pl.ds(first, count)]
        dst = pall.at[col if at is None else 2 * at + k, pl.ds(first, count)]
        pltpu.make_async_copy(src, dst, keep_sem.at[0]).start()
        over.start(src, dst, sibling)

    def goes_on(way, distance, chunk):
        return distance < 3 or (distance == 3 and (chunk < chunks // 2) == (way == 0))

    def pass_on(way, distance, chunk):
        here = part(held.at[z_of(way, distance)], chunk)
        ring[number(way, distance, chunk)].arrived(here, down if way == 0 else up)
        if goes_on(way, distance, chunk):
            ring[number(way, distance + 1, chunk)].start(here, here, up if way == 0 else down)
        if distance < 4 and chunk == chunks - 1:
            share(z_of(way, distance), 0, dens.shape[0])
        if distance == 4 and chunk % (chunks // 2) == chunks // 2 - 1:
            share(z_of(way, 4), way * (dens.shape[0] // 2), dens.shape[0] // 2)

    def ring_step(distance, chunk):
        for way in range(2):
            if distance < 4 or (chunk < chunks // 2) == (way == 0):
                pass_on(way, distance, chunk)

    steps = [(d, c) for d in (1, 2, 3) for c in range(chunks)] + [
        (4, c) for pair in range(chunks // 2) for c in (pair, pair + chunks // 2)
    ]

    def ring_end():
        over.arrived(pall.at[pl.ds(0, 8)], sibling)
        pltpu.make_async_copy(held, pall.at[pl.ds(0, 8)], keep_sem.at[0]).wait()

    def meet():
        code_step(3, "arrived")
        pcs, scs = pcode[...], scode[...]
        q = qc[None]
        match = ((pcs >> 3) == (q >> 3)) & ((scs >> 3) == (pcs & 7)) & ((scs & 7) == (q & 7))
        match = match & (pcs >= 0) & (scs >= 0) & (q >= 0)
        found = jnp.where(match, lax.broadcasted_iota(jnp.int32, (16, 8, B), 1) + 1, 0)
        found = jnp.sum(found, axis=1)
        source = lax.broadcasted_iota(jnp.int32, (B, B), 0)
        target = lax.broadcasted_iota(jnp.int32, (B, B), 1)

        def add_up(left, right):
            return jnp.dot(
                left.astype(jnp.bfloat16), right.astype(jnp.bfloat16), preferred_element_type=jnp.float32
            )

        def flag(condition):
            return condition.astype(jnp.float32)

        there = flag(found > 0)
        counts = add_up(there, flag((target == 64 + (source >> 3)) | (target == 72)))
        lane16 = lax.broadcasted_iota(jnp.int32, (16, B), 1)
        table_v[...] = jnp.where(lane16 < 64, found, counts.astype(jnp.int32))
        tile_to = lax.broadcasted_iota(jnp.int32, (16, 16), 0)
        tile_from = lax.broadcasted_iota(jnp.int32, (16, 16), 1)
        before = add_up(add_up(flag(tile_from < tile_to), there), flag(source >= 0))
        spot = before + add_up(there, flag(source <= target)) - 1.0
        spot = jnp.where((found > 0) & (spot < 128.0), spot, 255.0)
        spot = lax.dot_general(
            flag(source == target).astype(jnp.bfloat16), spot.astype(jnp.bfloat16), (((1,), (1,)), ((), ())),
            preferred_element_type=jnp.float32,
        ).astype(jnp.int32)
        tile16 = lax.broadcasted_iota(jnp.int32, (16, B), 0)
        high = (tile16 * 4 + (lane16 >> 4)).astype(jnp.float32)
        low = ((lane16 & 15) * 16 + found - 1).astype(jnp.float32)
        high_sum = jnp.zeros((1, B), jnp.float32)
        low_sum = jnp.zeros((1, B), jnp.float32)
        for t in range(16):
            hit = flag(spot[:, t : t + 1] == target)
            high_sum += add_up(high[t : t + 1], hit)
            low_sum += add_up(low[t : t + 1], hit)
        pairs_v[0:1, :] = high_sum.astype(jnp.int32) * 256 + low_sum.astype(jnp.int32)
        pairs_v[1:2, :] = add_up(flag(tile_from[0:8] >= 0), counts)[0:1].astype(jnp.int32)
        pltpu.make_async_copy(table_v, table, local_sem.at[3]).start()
        pltpu.make_async_copy(pairs_v, pairs, local_sem.at[4]).start()

    def density():
        for s in range(8):
            a = p_slots[s] >> 3
            b = p_slots[s] & 7
            left = own[a]
            right = jnp.concatenate([pan[i, b] for i in range(16)], axis=1)
            raw = lax.dot_general(left, right, (((1,), (1,)), ((), ())), preferred_element_type=jnp.float32)
            raw = jnp.where(jnp.full((B, B), p_count[0], jnp.int32) > s, raw, 0.0)
            dens[s] = raw.astype(jnp.bfloat16)
            if s % size == size - 1 and s >= size:
                ring_start(s // size - 1)
        ring_start(chunks - 1)
        share(None, 0, dens.shape[0])

    relays = [(j, side) for j in range(4) for side in range(2)]

    def inter_step(j, side):
        for half in range(2):
            inter.relay_second(half, j, side)

    def turn(core):
        def own(wave):
            for half in range(2):
                for chunk in range(2 * wave, 2 * wave + 2):
                    scattered(half, chunk)
                panel.first(2 * wave + half)
                panel.second(2 * wave + half, 0)

        def near(wave):
            for side in range(2):
                for half in range(2):
                    panel.relay_first(2 * wave + half, side)
                    panel.second(2 * wave + half, 1 + side)

        def far(wave):
            for half in range(2):
                panel.far_first(2 * wave + half)
                panel.second(2 * wave + half, 3)

        def onward(wave, j):
            for side in range(2):
                for half in range(2):
                    panel.relay_second(2 * wave + half, j, side)

        own(0)
        own(1)
        near(0)
        code_step(0, "arrived")
        code_step(1, "start")
        onward(0, 0)
        near(1)
        code_step(1, "arrived")
        code_step(2, "start")
        far(0)
        onward(0, 1)
        onward(0, 2)
        onward(1, 0)
        far(1)
        onward(1, 1)
        onward(1, 2)
        code_step(2, "arrived")
        code_step(3, "start")
        onward(0, 3)
        onward(1, 3)
        panel.far_second()
        for side in range(2):
            for half in range(2):
                inter.relay_first(half, side)
        for j in range(3):
            for half in range(2):
                inter.second(half, j)
        density()
        for n, step in enumerate(steps):
            ring_step(*step)
            if n == 0:
                for half in range(2):
                    inter.far_first(half)
                    inter.second(half, 3)
            if n == 1:
                meet()
            if 2 <= n < 2 + len(relays):
                inter_step(*relays[n - 2])
        inter.far_second()
        ring_end()
        keep_s.wait()
        pltpu.make_async_copy(table_v, table, local_sem.at[3]).wait()
        pltpu.make_async_copy(pairs_v, pairs, local_sem.at[4]).wait()
        panel.finish()
        inter.finish()
        all_sent(g_send, codes_sent, sibling)
        all_sent(z_send, held.at[pl.ds(0, 7)], sibling)
        all_sent(x_send, held, sibling)

    turn(2)

    for piece in pieces:

        def left(sems, piece=piece):
            whole = relay.at[piece.e]
            pltpu.make_async_remote_copy(
                src_ref=whole, dst_ref=whole, send_sem=sems.at[piece.e], recv_sem=sems.at[piece.e],
                device_id=sibling, device_id_type=MESH,
            ).wait_send()

        piece.moved(functools.partial(left, plane_send))
        pl.when(piece.peer != col)(functools.partial(left, far_send))


def product_kernel(pairs, table, pall, sall, out, dens, sidx, todo, pbuf, sbuf, count, sem, sem_p, sem_s):
    depth = pbuf.shape[0]
    col = lax.axis_index("col")
    keep = pltpu.make_async_copy(pall.at[col], dens, sem.at[0])
    keep.start()
    total = pairs[1, 72]
    count[0] = total

    def copies(i, code):
        t, p, s = code // 1024, code // 128 % 8, code % 16
        at = i % depth
        return (
            pltpu.make_async_copy(pall.at[t, p], pbuf.at[at], sem_p.at[at]),
            pltpu.make_async_copy(sall.at[t, s], sbuf.at[at], sem_s.at[at]),
        )

    def begin(i, code):
        for copy in copies(i, code):
            copy.start()

    def tile(t, _):
        @pl.when(sidx[t, 72] > 0)
        def _():
            def slot(p, _):
                @pl.when(sidx[t, 64 + p] > 0)
                def _():
                    def pair(q, _):
                        v = sidx[t, 8 * p + q]

                        @pl.when(v > 0)
                        def _():
                            n = count[0]
                            code = t * 1024 + p * 128 + q * 16 + v - 1
                            todo[n] = code
                            count[0] = n + 1

                            @pl.when(n < depth)
                            def _():
                                begin(n, code)

                        return 0

                    lax.fori_loop(0, 8, pair, 0)

                return 0

            lax.fori_loop(0, 8, slot, 0)

        return 0

    def listed(i, _):
        code = pairs[0, i]
        todo[i] = code

        @pl.when(i < depth)
        def _():
            begin(i, code)

        return 0

    @pl.when(total <= LISTED)
    def _():
        lax.fori_loop(0, total, listed, 0)

    @pl.when(total > LISTED)
    def _():
        fetch = pltpu.make_async_copy(table, sidx, sem.at[1])
        fetch.start()
        fetch.wait()
        count[0] = 0
        lax.fori_loop(0, 16, tile, 0)

    n = count[0]
    out[...] = jnp.zeros_like(out)

    def work(first, size):
        sums = []
        for i in [first + g for g in range(size)]:
            code = todo[i]
            for copy in copies(i, code):
                copy.wait()
            at = i % depth
            sums.append((code // 16 % 8, jnp.dot(pbuf[at], sbuf[at], preferred_element_type=jnp.float32)))
        for g, (q, block) in enumerate(sums):
            out[q] += block

            @pl.when(first + g + depth < n)
            def _(g=g):
                begin(first + g + depth, todo[first + g + depth])

        return 0

    lax.fori_loop(0, n // 4, lambda i, _: work(4 * i, 4), 0)
    lax.fori_loop(n // 4 * 4, n, lambda i, _: work(i, 1), 0)
    keep.wait()


def on_device(coeffs, p_slots, p_count, s_blocks, s_slots, s_count, q_slots, q_count):
    rows, orbitals = coeffs.shape
    n = 16
    smem = pl.BlockSpec(memory_space=pltpu.SMEM)
    vmem = pl.BlockSpec(memory_space=pltpu.VMEM)
    anyspace = pl.BlockSpec(memory_space=pl.ANY)
    gathered = jax.ShapeDtypeStruct((n, rows // B, B, B), jnp.bfloat16)
    dma = pltpu.SemaphoreType.DMA
    pall, sall, pairs, table = pl.pallas_call(
        gather_kernel,
        out_shape=(
            gathered, gathered, jax.ShapeDtypeStruct((8, B), jnp.int32), jax.ShapeDtypeStruct((n, B), jnp.int32),
        ),
        in_specs=[anyspace] * 8,
        out_specs=(anyspace, anyspace, anyspace, anyspace),
        scratch_shapes=[
            *[pltpu.SMEM((size,), jnp.int32) for size in (8, 1) * 3],
            pltpu.VMEM((rows // B, B, orbitals), jnp.bfloat16),
            pltpu.VMEM((n, rows // B, B, B), jnp.bfloat16),
            pltpu.VMEM((rows // B, B, B), jnp.bfloat16),
            pltpu.VMEM((rows // B, B, B), jnp.bfloat16),
            pltpu.VMEM((8, rows // B, B, B), jnp.bfloat16),
            pltpu.VMEM((2, rows // B // 2, B, B), jnp.bfloat16),
            pltpu.VMEM((2 * n, 8, B), jnp.int32),
            pltpu.VMEM((8, B), jnp.int32),
            pltpu.VMEM((n, B), jnp.int32),
            dma((5,)), dma((2,)), dma((2, 4)), dma((2,)), dma((2, 4)),
            dma((1,)), dma((49,)), dma((1,)), dma((8,)), dma((1,)), dma((25,)), dma((1,)), dma((28,)),
            dma((1,)), dma((1,)), dma((1,)), dma((6,)),
        ],
        compiler_params=pltpu.CompilerParams(collective_id=0, has_side_effects=True),
        name="gather",
    )(
        coeffs.reshape(rows // B, B, orbitals), s_blocks.reshape(rows // B, B, B), p_slots.reshape(8), p_count.reshape(1), s_slots.reshape(8),
        s_count.reshape(1), q_slots.reshape(8), q_count.reshape(1),
    )
    depth = 32
    product, dens = pl.pallas_call(
        product_kernel,
        out_shape=(
            jax.ShapeDtypeStruct((8, B, B), jnp.float32), jax.ShapeDtypeStruct((8, B, B), jnp.bfloat16)
        ),
        in_specs=[smem, anyspace, anyspace, anyspace],
        out_specs=(vmem, vmem),
        scratch_shapes=[
            pltpu.SMEM((n, B), jnp.int32),
            pltpu.SMEM((1024,), jnp.int32),
            pltpu.VMEM((depth, B, B), jnp.bfloat16),
            pltpu.VMEM((depth, B, B), jnp.bfloat16),
            pltpu.SMEM((1,), jnp.int32),
            dma((2,)), dma((depth,)), dma((depth,)),
        ],
        name="product",
    )(pairs, table, pall, sall)
    return dens.reshape(1, 1, 8, B, B), product.reshape(1, 1, 8, B, B)


def solution(mesh):
    return jax.shard_map(
        on_device,
        mesh=mesh,
        in_specs=(
            P("row", None),
            P("row", "col", None),
            P("row", "col"),
            P("row", "col", None, None, None),
            P("row", "col", None),
            P("row", "col"),
            P("row", "col", None),
            P("row", "col"),
        ),
        out_specs=(P("row", "col", None, None, None), P("row", "col", None, None, None)),
        check_vma=False,
    )
```

```python
import functools

import jax
import jax.numpy as jnp
from jax import lax
from jax.experimental import pallas as pl
from jax.experimental.pallas import tpu as pltpu
from jax.sharding import PartitionSpec as P

MESH = pl.DeviceIdType.MESH
B = 128
LISTED = 128
FIRST = (8, 11, 6, 9, 14, 7, 10, 5)
SECOND = (2, 1, 12, 3, 4, 13, 0, 15)
PLANE = tuple((FIRST if i in FIRST else SECOND).index(i) for i in range(16))


def lookup(table, at):
    value = 0
    for base in range(0, len(table), 4):
        packed = sum(table[base + i] << (4 * i) for i in range(4))
        inside = (at // 4 == base // 4).astype(jnp.int32)
        value = value + inside * ((packed // (1 << (4 * (at % 4)))) % 16)
    return value


class Link:
    def __init__(self, send, recv, at):
        self.send, self.recv, self.at = send, recv, at

    def start(self, src, dst, device):
        pltpu.make_async_remote_copy(
            src_ref=src, dst_ref=dst, send_sem=self.send.at[0], recv_sem=self.recv.at[self.at],
            device_id=device, device_id_type=MESH,
        ).start()

    def arrived(self, landing, device):
        pltpu.make_async_remote_copy(
            src_ref=landing, dst_ref=landing, send_sem=self.send.at[0], recv_sem=self.recv.at[self.at],
            device_id=device, device_id_type=MESH,
        ).wait_recv()


def all_sent(send, whole, device):
    pltpu.make_async_remote_copy(
        src_ref=whole, dst_ref=whole, send_sem=send.at[0], recv_sem=send.at[0], device_id=device, device_id_type=MESH
    ).wait_send()


class PlaneGather:
    def __init__(self, buf, own, send, recv, place, streams):
        self.buf, self.own = buf, own
        self.y, self.x, self.col = place
        self.size = own.shape[0] // streams
        self.links = [Link(send, recv, m) for m in range(12 * streams + 1)]

    def index(self, stream, du, dv):
        if stream % 2 == 0:
            return 4 * ((self.y + dv + 4) % 4) + (self.x + du + 4) % 4
        return 4 * ((self.y + du + 4) % 4) + (self.x + dv + 4) % 4

    def device(self, stream, du, dv):
        return (self.index(stream, du, dv), self.col)

    def span(self, stream, part):
        base = (stream % 2) * self.own.shape[0] // 2 + (stream // 2) * self.size
        if part is None:
            return pl.ds(base, self.size)
        return pl.ds(base + part * (self.size // 2), self.size // 2)

    def block(self, stream, du, dv, part=None):
        return self.buf.at[self.index(stream, du, dv), self.span(stream, part)]

    def link(self, stream, number):
        return self.links[12 * stream + number]

    def first(self, stream):
        src = self.own.at[self.span(stream, None)]
        dst = self.block(stream, 0, 0)
        self.link(stream, 0).start(src, dst, self.device(stream, 1, 0))
        self.link(stream, 1).start(src, dst, self.device(stream, -1, 0))

    def relay_first(self, stream, side):
        du = -1 if side == 0 else 1
        self.link(stream, side).arrived(self.block(stream, du, 0), self.device(stream, du, 0))
        part = self.block(stream, du, 0, side)
        self.link(stream, 2 + side).start(part, part, self.device(stream, -du, 0))

    def far_first(self, stream):
        for side in range(2):
            part = self.block(stream, 2, 0, side)
            self.link(stream, 2 + side).arrived(part, self.device(stream, -1 if side == 0 else 1, 0))

    def second(self, stream, j):
        du = (0, -1, 1, 2)[j]
        dst = self.block(stream, du, 0)
        src = self.own.at[self.span(stream, None)] if j == 0 else dst
        self.link(stream, 4 + 2 * j).start(src, dst, self.device(stream, 0, 1))
        self.link(stream, 5 + 2 * j).start(src, dst, self.device(stream, 0, -1))

    def relay_second(self, stream, j, side):
        du = (0, -1, 1, 2)[j]
        dv = -1 if side == 0 else 1
        number = 4 + 2 * j + side
        self.link(stream, number).arrived(self.block(stream, du, dv), self.device(stream, 0, dv))
        part = self.block(stream, du, dv, side)
        self.links[-1].start(part, part, self.device(stream, 0, -dv))

    def far_second(self):
        self.links[-1].arrived(self.buf.at[pl.ds(0, 4)], self.device(0, 0, 1))

    def finish(self):
        all_sent(self.links[0].send, self.buf.at[pl.ds(0, 15)], self.device(0, 1, 0))


def gather_kernel(
    coeffs, sblk, p_slots_in, p_count_in, s_slots_in, s_count_in, q_slots_in, q_count_in,
    pall, sall, pairs, table,
    p_slots, p_count, s_slots, s_count, q_slots, q_count,
    own, pan, sown, dens, held, relay, code_v, pairs_v, table_v,
    local_sem, plane_send, plane_recv, far_send, far_recv, c_send, c_recv, g_send, g_recv, s_send, s_recv, z_send, z_recv,
    x_send, x_recv, keep_sem, small_sem,
):
    row = lax.axis_index("row")
    col = lax.axis_index("col")
    pcode, scode = code_v.at[pl.ds(0, 16)], code_v.at[pl.ds(16, 16)]
    codes_sent = code_v.at[pl.ds(0, 30)]
    y, x = row // 4, row % 4
    z, k = col // 2, col % 2

    load_own = pltpu.make_async_copy(coeffs, own, local_sem.at[0])
    load_s = pltpu.make_async_copy(sblk, sown, local_sem.at[1])

    barrier = pltpu.get_barrier_semaphore()
    for j in range(1, 16):
        pl.semaphore_signal(barrier, inc=1, device_id=(row, (col + j) % 16), device_id_type=MESH)
        pl.semaphore_signal(barrier, inc=1, device_id=((row + j) % 16, col), device_id_type=MESH)

    load_own.start()
    load_s.start()
    small = [
        pltpu.make_async_copy(src, dst, small_sem.at[at])
        for at, (src, dst) in enumerate((
            (p_slots_in, p_slots), (p_count_in, p_count), (s_slots_in, s_slots),
            (s_count_in, s_count), (q_slots_in, q_slots), (q_count_in, q_count),
        ))
    ]
    for copy in small:
        copy.start()
    for copy in small:
        copy.wait()

    lane = lax.broadcasted_iota(jnp.int32, (8, B), 1)
    sub = lax.broadcasted_iota(jnp.int32, (8, B), 0)
    pc = jnp.full((8, B), -1, jnp.int32)
    qc = jnp.full((8, B), -100, jnp.int32)
    sc = jnp.full((8, B), -1, jnp.int32)
    p_live = jnp.full((8, B), p_count[0], jnp.int32)
    q_live = jnp.full((8, B), q_count[0], jnp.int32)
    s_live = jnp.full((8, B), s_count[0], jnp.int32)
    for i in range(8):
        pc = jnp.where((lane // 8 == i) & (p_live > i), jnp.full((8, B), p_slots[i], jnp.int32), pc)
        qc = jnp.where(
            (lane % 8 == i) & (lane < 64) & (q_live > i), jnp.full((8, B), q_slots[i], jnp.int32), qc
        )
        sc = jnp.where((sub == i) & (s_live > i), jnp.full((8, B), s_slots[i], jnp.int32), sc)
    pcode[col] = pc
    scode[row] = sc

    load_own.wait()
    load_s.wait()

    pl.semaphore_wait(barrier, 30)

    def slice_of(at, chunk):
        return own.at[4 * k + chunk, :, pl.ds(pl.multiple_of(at * B, B), B)]

    class Piece:
        def __init__(self, e, table):
            self.shift = lookup(table, z)
            self.e, self.moves = e, 0 not in table
            self.peer = row ^ self.shift

        def copy_in_plane(self, chunk):
            return pltpu.make_async_remote_copy(
                src_ref=slice_of(self.peer, chunk), dst_ref=relay.at[self.e, chunk],
                send_sem=plane_send.at[self.e], recv_sem=plane_recv.at[self.e, chunk],
                device_id=(self.peer, col), device_id_type=MESH,
            )

        def moved(self, act):
            if self.moves:
                act()
            else:
                pl.when(self.shift != 0)(act)

        def stays(self, act):
            if not self.moves:
                pl.when(self.shift == 0)(act)

        def far(self, src, chunk):
            return pltpu.make_async_remote_copy(
                src_ref=src, dst_ref=pan.at[row, 4 * k + chunk],
                send_sem=far_send.at[self.e], recv_sem=far_recv.at[k, chunk],
                device_id=(row, self.peer), device_id_type=MESH,
            )

        def hand_on(self, src, chunk):
            @pl.when(self.peer == col)
            def _():
                pltpu.make_async_copy(src, pan.at[row, 4 * k + chunk], far_recv.at[k, chunk]).start()

            @pl.when(self.peer != col)
            def _():
                self.far(src, chunk).start()

    pieces = [Piece(0, FIRST), Piece(1, SECOND)]
    for chunk in range(4):
        for piece in pieces:
            piece.moved(lambda piece=piece, chunk=chunk: piece.copy_in_plane(chunk).start())
            piece.stays(lambda piece=piece, chunk=chunk: piece.hand_on(slice_of(row, chunk), chunk))

    place = (y, x, col)
    panel = PlaneGather(pan, pan.at[row], c_send, c_recv, place, 4)
    inter = PlaneGather(sall, sown, s_send, s_recv, place, 2)
    keep_s = pltpu.make_async_copy(sown, sall.at[row], local_sem.at[2])
    keep_s.start()

    for chunk in range(4):
        for piece in pieces:

            def pass_along(piece=piece, chunk=chunk):
                piece.copy_in_plane(chunk).wait_recv()
                piece.hand_on(relay.at[piece.e, chunk], chunk)

            piece.moved(pass_along)

    for half in range(2):
        inter.first(half)
    codes = [Link(g_send, g_recv, m) for m in range(8)]

    def code_step(step, act):
        size = 1 << step
        for dim, (ref, me) in enumerate(((pcode, col), (scode, row))):
            mine = me // size * size
            other = me ^ size
            device = (row, other) if dim == 0 else (other, col)
            if act == "start":
                here = ref.at[pl.ds(mine, size)]
                codes[2 * step + dim].start(here, here, device)
            else:
                codes[2 * step + dim].arrived(ref.at[pl.ds(mine ^ size, size)], device)

    code_step(0, "start")

    my_plane = lookup(PLANE, row ^ col)

    def scattered(half, chunk):
        by_me = (my_plane == z) & (k == half)
        landing = pan.at[row, 4 * half + chunk]

        @pl.when(by_me)
        def _():
            pltpu.make_async_copy(landing, landing, far_recv.at[half, chunk]).wait()

        @pl.when(jnp.logical_not(by_me))
        def _():
            pltpu.make_async_remote_copy(
                src_ref=landing, dst_ref=landing, send_sem=far_send.at[0],
                recv_sem=far_recv.at[half, chunk],
                device_id=(row, col + 1 - 2 * k), device_id_type=MESH,
            ).wait_recv()

    sibling = (row, col + 1 - 2 * k)
    up = (row, (col + 2) % 16)
    down = (row, (col + 14) % 16)
    chunks = 4
    size = dens.shape[0] // chunks
    ring = [Link(z_send, z_recv, m) for m in range(7 * chunks)]
    over = Link(x_send, x_recv, 0)

    def number(way, distance, chunk):
        return 7 * chunks // 2 * way + (
            chunks * (distance - 1) + chunk if distance < 4 else 3 * chunks + chunk % (chunks // 2)
        )

    def z_of(way, distance):
        return (z + 8 - distance) % 8 if way == 0 else (z + distance) % 8

    def part(ref, chunk):
        return ref.at[pl.ds(chunk * size, size)]

    def ring_start(chunk):
        for way in range(2):
            ring[number(way, 1, chunk)].start(
                part(dens, chunk), part(held.at[z], chunk), up if way == 0 else down
            )

    def share(at, first, count):
        src = (dens if at is None else held.at[at]).at[pl.ds(first, count)]
        dst = pall.at[col if at is None else 2 * at + k, pl.ds(first, count)]
        pltpu.make_async_copy(src, dst, keep_sem.at[0]).start()
        over.start(src, dst, sibling)

    def goes_on(way, distance, chunk):
        return distance < 3 or (distance == 3 and (chunk < chunks // 2) == (way == 0))

    def pass_on(way, distance, chunk):
        here = part(held.at[z_of(way, distance)], chunk)
        ring[number(way, distance, chunk)].arrived(here, down if way == 0 else up)
        if goes_on(way, distance, chunk):
            ring[number(way, distance + 1, chunk)].start(here, here, up if way == 0 else down)
        if distance < 4 and chunk == chunks - 1:
            share(z_of(way, distance), 0, dens.shape[0])
        if distance == 4 and chunk % (chunks // 2) == chunks // 2 - 1:
            share(z_of(way, 4), way * (dens.shape[0] // 2), dens.shape[0] // 2)

    def ring_step(distance, chunk):
        for way in range(2):
            if distance < 4 or (chunk < chunks // 2) == (way == 0):
                pass_on(way, distance, chunk)

    steps = [(d, c) for d in (1, 2, 3) for c in range(chunks)] + [
        (4, c) for pair in range(chunks // 2) for c in (pair, pair + chunks // 2)
    ]

    def ring_end():
        over.arrived(pall.at[pl.ds(0, 8)], sibling)
        pltpu.make_async_copy(held, pall.at[pl.ds(0, 8)], keep_sem.at[0]).wait()

    def meet():
        code_step(3, "arrived")
        pcs, scs = pcode[...], scode[...]
        q = qc[None]
        match = ((pcs >> 3) == (q >> 3)) & ((scs >> 3) == (pcs & 7)) & ((scs & 7) == (q & 7))
        match = match & (pcs >= 0) & (scs >= 0) & (q >= 0)
        found = jnp.where(match, lax.broadcasted_iota(jnp.int32, (16, 8, B), 1) + 1, 0)
        found = jnp.sum(found, axis=1)
        source = lax.broadcasted_iota(jnp.int32, (B, B), 0)
        target = lax.broadcasted_iota(jnp.int32, (B, B), 1)

        def add_up(left, right):
            return jnp.dot(
                left.astype(jnp.bfloat16), right.astype(jnp.bfloat16), preferred_element_type=jnp.float32
            )

        def flag(condition):
            return condition.astype(jnp.float32)

        there = flag(found > 0)
        counts = add_up(there, flag((target == 64 + (source >> 3)) | (target == 72)))
        lane16 = lax.broadcasted_iota(jnp.int32, (16, B), 1)
        table_v[...] = jnp.where(lane16 < 64, found, counts.astype(jnp.int32))
        tile_to = lax.broadcasted_iota(jnp.int32, (16, 16), 0)
        tile_from = lax.broadcasted_iota(jnp.int32, (16, 16), 1)
        before = add_up(add_up(flag(tile_from < tile_to), there), flag(source >= 0))
        spot = before + add_up(there, flag(source <= target)) - 1.0
        spot = jnp.where((found > 0) & (spot < 128.0), spot, 255.0)
        spot = lax.dot_general(
            flag(source == target).astype(jnp.bfloat16), spot.astype(jnp.bfloat16), (((1,), (1,)), ((), ())),
            preferred_element_type=jnp.float32,
        ).astype(jnp.int32)
        tile16 = lax.broadcasted_iota(jnp.int32, (16, B), 0)
        high = (tile16 * 4 + (lane16 >> 4)).astype(jnp.float32)
        low = ((lane16 & 15) * 16 + found - 1).astype(jnp.float32)
        high_sum = jnp.zeros((1, B), jnp.float32)
        low_sum = jnp.zeros((1, B), jnp.float32)
        for t in range(16):
            hit = flag(spot[:, t : t + 1] == target)
            high_sum += add_up(high[t : t + 1], hit)
            low_sum += add_up(low[t : t + 1], hit)
        pairs_v[0:1, :] = high_sum.astype(jnp.int32) * 256 + low_sum.astype(jnp.int32)
        pairs_v[1:2, :] = add_up(flag(tile_from[0:8] >= 0), counts)[0:1].astype(jnp.int32)
        pltpu.make_async_copy(table_v, table, local_sem.at[3]).start()
        pltpu.make_async_copy(pairs_v, pairs, local_sem.at[4]).start()

    def density():
        for s in range(8):
            a = p_slots[s] >> 3
            b = p_slots[s] & 7
            left = own[a]
            right = jnp.concatenate([pan[i, b] for i in range(16)], axis=1)
            raw = lax.dot_general(left, right, (((1,), (1,)), ((), ())), preferred_element_type=jnp.float32)
            raw = jnp.where(jnp.full((B, B), p_count[0], jnp.int32) > s, raw, 0.0)
            dens[s] = raw.astype(jnp.bfloat16)
            if s % size == size - 1 and s >= size:
                ring_start(s // size - 1)
        ring_start(chunks - 1)
        share(None, 0, dens.shape[0])

    relays = [(j, side) for j in range(4) for side in range(2)]

    def inter_step(j, side):
        for half in range(2):
            inter.relay_second(half, j, side)

    def turn(core):
        def own(wave):
            for half in range(2):
                for chunk in range(2 * wave, 2 * wave + 2):
                    scattered(half, chunk)
                panel.first(2 * wave + half)
                panel.second(2 * wave + half, 0)

        def near(wave):
            for side in range(2):
                for half in range(2):
                    panel.relay_first(2 * wave + half, side)
                    panel.second(2 * wave + half, 1 + side)

        def far(wave):
            for half in range(2):
                panel.far_first(2 * wave + half)
                panel.second(2 * wave + half, 3)

        def onward(wave, j):
            for side in range(2):
                for half in range(2):
                    panel.relay_second(2 * wave + half, j, side)

        own(0)
        own(1)
        near(0)
        code_step(0, "arrived")
        code_step(1, "start")
        onward(0, 0)
        near(1)
        code_step(1, "arrived")
        code_step(2, "start")
        far(0)
        onward(0, 1)
        onward(0, 2)
        onward(1, 0)
        far(1)
        onward(1, 1)
        onward(1, 2)
        code_step(2, "arrived")
        code_step(3, "start")
        onward(0, 3)
        onward(1, 3)
        panel.far_second()
        for side in range(2):
            for half in range(2):
                inter.relay_first(half, side)
        for j in range(3):
            for half in range(2):
                inter.second(half, j)
        density()
        for n, step in enumerate(steps):
            ring_step(*step)
            if n == 0:
                for half in range(2):
                    inter.far_first(half)
                    inter.second(half, 3)
            if n == 1:
                meet()
            if 2 <= n < 2 + len(relays):
                inter_step(*relays[n - 2])
        inter.far_second()
        ring_end()
        keep_s.wait()
        pltpu.make_async_copy(table_v, table, local_sem.at[3]).wait()
        pltpu.make_async_copy(pairs_v, pairs, local_sem.at[4]).wait()
        panel.finish()
        inter.finish()
        all_sent(g_send, codes_sent, sibling)
        all_sent(z_send, held.at[pl.ds(0, 7)], sibling)
        all_sent(x_send, held, sibling)

    turn(2)

    for piece in pieces:

        def left(sems, piece=piece):
            whole = relay.at[piece.e]
            pltpu.make_async_remote_copy(
                src_ref=whole, dst_ref=whole, send_sem=sems.at[piece.e], recv_sem=sems.at[piece.e],
                device_id=sibling, device_id_type=MESH,
            ).wait_send()

        piece.moved(functools.partial(left, plane_send))
        pl.when(piece.peer != col)(functools.partial(left, far_send))


def product_kernel(pairs_in, table, pall, sall, out, dens, pairs, held, sidx, todo, pbuf, sbuf, count, sem, sem_p, sem_s):
    depth = pbuf.shape[0]
    col = lax.axis_index("col")
    fetch_pairs = pltpu.make_async_copy(pairs_in, pairs, sem.at[2])
    fetch_pairs.start()
    take = pltpu.make_async_copy(pall.at[col], held, sem.at[0])
    take.start()
    out[...] = jnp.zeros_like(out)
    fetch_pairs.wait()
    total = pairs[1, 72]
    count[0] = total

    def copies(i, code):
        t, p, s = code // 1024, code // 128 % 8, code % 16
        at = i % depth
        return (
            pltpu.make_async_copy(pall.at[t, p], pbuf.at[at], sem_p.at[at]),
            pltpu.make_async_copy(sall.at[t, s], sbuf.at[at], sem_s.at[at]),
        )

    def begin(i, code):
        for copy in copies(i, code):
            copy.start()

    def tile(t, _):
        @pl.when(sidx[t, 72] > 0)
        def _():
            def slot(p, _):
                @pl.when(sidx[t, 64 + p] > 0)
                def _():
                    def pair(q, _):
                        v = sidx[t, 8 * p + q]

                        @pl.when(v > 0)
                        def _():
                            n = count[0]
                            code = t * 1024 + p * 128 + q * 16 + v - 1
                            todo[n] = code
                            count[0] = n + 1

                            @pl.when(n < depth)
                            def _():
                                begin(n, code)

                        return 0

                    lax.fori_loop(0, 8, pair, 0)

                return 0

            lax.fori_loop(0, 8, slot, 0)

        return 0

    def listed(i, _):
        code = pairs[0, i]
        todo[i] = code

        @pl.when(i < depth)
        def _():
            begin(i, code)

        return 0

    @pl.when(total <= LISTED)
    def _():
        lax.fori_loop(0, total, listed, 0)

    @pl.when(total > LISTED)
    def _():
        fetch = pltpu.make_async_copy(table, sidx, sem.at[1])
        fetch.start()
        fetch.wait()
        count[0] = 0
        lax.fori_loop(0, 16, tile, 0)

    n = count[0]
    take.wait()
    keep = pltpu.make_async_copy(held, dens, sem.at[3])
    keep.start()

    def work(first, size):
        sums = []
        for i in [first + g for g in range(size)]:
            code = todo[i]
            for copy in copies(i, code):
                copy.wait()
            at = i % depth
            sums.append((code // 16 % 8, jnp.dot(pbuf[at], sbuf[at], preferred_element_type=jnp.float32)))
        for g, (q, block) in enumerate(sums):
            out[q] += block

            @pl.when(first + g + depth < n)
            def _(g=g):
                begin(first + g + depth, todo[first + g + depth])

        return 0

    lax.fori_loop(0, n // 4, lambda i, _: work(4 * i, 4), 0)
    lax.fori_loop(n // 4 * 4, n, lambda i, _: work(i, 1), 0)
    keep.wait()


def on_device(coeffs, p_slots, p_count, s_blocks, s_slots, s_count, q_slots, q_count):
    rows, orbitals = coeffs.shape
    n = 16
    vmem = pl.BlockSpec(memory_space=pltpu.VMEM)
    anyspace = pl.BlockSpec(memory_space=pl.ANY)
    gathered = jax.ShapeDtypeStruct((n, rows // B, B, B), jnp.bfloat16)
    dma = pltpu.SemaphoreType.DMA
    pall, sall, pairs, table = pl.pallas_call(
        gather_kernel,
        out_shape=(
            gathered, gathered, jax.ShapeDtypeStruct((8, B), jnp.int32), jax.ShapeDtypeStruct((n, B), jnp.int32),
        ),
        in_specs=[anyspace] * 8,
        out_specs=(anyspace, anyspace, anyspace, anyspace),
        scratch_shapes=[
            *[pltpu.SMEM((size,), jnp.int32) for size in (8, 1) * 3],
            pltpu.VMEM((rows // B, B, orbitals), jnp.bfloat16),
            pltpu.VMEM((n, rows // B, B, B), jnp.bfloat16),
            pltpu.VMEM((rows // B, B, B), jnp.bfloat16),
            pltpu.VMEM((rows // B, B, B), jnp.bfloat16),
            pltpu.VMEM((8, rows // B, B, B), jnp.bfloat16),
            pltpu.VMEM((2, rows // B // 2, B, B), jnp.bfloat16),
            pltpu.VMEM((2 * n, 8, B), jnp.int32),
            pltpu.VMEM((8, B), jnp.int32),
            pltpu.VMEM((n, B), jnp.int32),
            dma((5,)), dma((2,)), dma((2, 4)), dma((2,)), dma((2, 4)),
            dma((1,)), dma((49,)), dma((1,)), dma((8,)), dma((1,)), dma((25,)), dma((1,)), dma((28,)),
            dma((1,)), dma((1,)), dma((1,)), dma((6,)),
        ],
        compiler_params=pltpu.CompilerParams(collective_id=0, has_side_effects=True),
        name="gather",
    )(
        coeffs.reshape(rows // B, B, orbitals), s_blocks.reshape(rows // B, B, B), p_slots.reshape(8), p_count.reshape(1), s_slots.reshape(8),
        s_count.reshape(1), q_slots.reshape(8), q_count.reshape(1),
    )
    depth = 32
    product, dens = pl.pallas_call(
        product_kernel,
        out_shape=(
            jax.ShapeDtypeStruct((8, B, B), jnp.float32), jax.ShapeDtypeStruct((8, B, B), jnp.bfloat16)
        ),
        in_specs=[anyspace, anyspace, anyspace, anyspace],
        out_specs=(vmem, anyspace),
        scratch_shapes=[
            pltpu.SMEM((8, B), jnp.int32),
            pltpu.VMEM((8, B, B), jnp.bfloat16),
            pltpu.SMEM((n, B), jnp.int32),
            pltpu.SMEM((1024,), jnp.int32),
            pltpu.VMEM((depth, B, B), jnp.bfloat16),
            pltpu.VMEM((depth, B, B), jnp.bfloat16),
            pltpu.SMEM((1,), jnp.int32),
            dma((4,)), dma((depth,)), dma((depth,)),
        ],
        name="product",
    )(pairs, table, pall, sall)
    return dens.reshape(1, 1, 8, B, B), product.reshape(1, 1, 8, B, B)


def solution(mesh):
    return jax.shard_map(
        on_device,
        mesh=mesh,
        in_specs=(
            P("row", None),
            P("row", "col", None),
            P("row", "col"),
            P("row", "col", None, None, None),
            P("row", "col", None),
            P("row", "col"),
            P("row", "col", None),
            P("row", "col"),
        ),
        out_specs=(P("row", "col", None, None, None), P("row", "col", None, None, None)),
        check_vma=False,
    )
```
